256 devices in a mesh: dp: 8 (over z), expert: 8 (over x, core), mp: 4 (over y).
Axes of the slice: x: 4, y: 4, z: 8, core: 2. Of those that a mesh axis runs over, the one named last changes fastest.
Arguments:
- queries: bfloat16 [256, 4096], P('dp', 'expert'), may hold values from -6 to 6
- fresh_entries: bfloat16 [2, 256, 1024], P(None, 'dp', 'expert'), may hold values from -6 to 6
- page_cache: bfloat16 [8, 1024, 2, 256, 128], P('expert', ('dp', 'mp')), may hold values from -6 to 6
- lengths: int32 [256], replicated, may hold values from 2 to 1024, as said below
- page_holder: int32 [256, 4], replicated, may hold values from 0 to 31, as said below
- page_slot: int32 [256, 4], replicated, may hold values from 0 to 31, as said below
- tokens: bfloat16 [256, 4096], P('dp'), may hold values from -6 to 6
- norm_gain: float32 [4096], replicated, may hold values from 0.5 to 1.5
- out_weight: bfloat16 [4096, 4096], P(('expert', 'mp')), may hold values from -0.09375 to 0.09375
- expert_ids: int32 [256, 2], replicated, may hold values from 0 to 7, all different within a row; in each aligned block of 32 rows (0 to 31, 32 to 63, ...) at most 16 rows name the same one
- gate_values: float32 [256, 2], replicated, may hold values from 0.1 to 0.9
- gate_weight: bfloat16 [8, 4096, 8192], P('expert', None, ('dp', 'mp')), may hold values from -0.09375 to 0.09375
- up_weight: bfloat16 [8, 4096, 8192], P('expert', None, ('dp', 'mp')), may hold values from -0.09375 to 0.09375
- down_weight: bfloat16 [8, 8192, 4096], P('expert', ('dp', 'mp')), may hold values from -0.0625 to 0.0625
Outputs:
- layer_output: bfloat16 [256, 4096], P(('dp', 'expert', 'mp'))
The draws below stay inside these ranges and needn't reach their ends.
Inputs may be any that keep to these rules, and one draw needn't show every extreme that they name: `lengths`: cached positions of each sequence; sequences of one dp index share a most that is a multiple of 256 and is reached by one of them. `page_holder`: number the sequences in aligned blocks of 32; within one block, among the pages whose index has one remainder modulo 4, every holder index occurs exactly 1 times. `page_slot`: no two pages of all sequences share both holder and slot. `expert_ids`: each row names 2 different experts; in each aligned block of 32 rows no expert is named more than 16 times.
All inputs are finite; a program needn't handle non-finite values.
Results may differ from the reference program's by a relative error of at most 0.014.
Values may be sent and summed in bfloat16 or wider, within the bound.
No kernel may reach another device: no remote copies, remote signals or barrier semaphores. Data moves between devices by JAX's collectives and lax.ppermute only.
A program may use at most 64 MiB of HBM per device.

```python
import math
import jax
import jax.numpy as jnp
import numpy as np
from jax import lax

D = 4096
QUERY_HEADS = 32
KEY_VALUE_HEADS = 8
HEAD_WIDTH = 128
E = 8
TOPK = 2
FF = 8192
PAGE_LENGTH = 256
PMAX = 4
SEQ_DP = 32
SEQUENCE_TOTAL = 256
P_OWN = 32
CAPP = 1
HOLDER_SLOTS = 32
CAP = 16
N_DP = 8
N_MP = 4


def permute_count(subkey, length):
    return jax.random.permutation(subkey, length)


def page_table(key):
    base_key = jax.random.fold_in(key, 17)
    holders = N_DP * N_MP
    owner_keys = jax.random.split(jax.random.fold_in(base_key, 1), holders)
    per_owner = jax.vmap(partial_owner)(owner_keys)
    holder_index = per_owner // CAPP
    ranking = per_owner % CAPP
    holder_keys = jax.random.split(jax.random.fold_in(base_key, 2), holders)
    per_holder = jax.vmap(partial_holder)(holder_keys)
    owner_index = jnp.arange(holders, dtype=jnp.int32)[:, None]
    slot_index = per_holder[holder_index, owner_index * CAPP + ranking]
    return (arrange_table(holder_index), arrange_table(slot_index))


def partial_owner(subkey):
    return permute_count(subkey, P_OWN).astype(jnp.int32)


def partial_holder(subkey):
    return permute_count(subkey, HOLDER_SLOTS).astype(jnp.int32)


def arrange_table(entries):
    shaped = entries.reshape(N_DP, N_MP, SEQ_DP, P_OWN // SEQ_DP)
    return shaped.transpose(0, 2, 3, 1).reshape(SEQUENCE_TOTAL, PMAX).astype(jnp.int32)


def draw_page_holder(key, part):
    return page_table(key)[0]


def draw_page_slot(key, part):
    return page_table(key)[1]


def draw_lengths(key, part):
    page_limits = jax.random.randint(jax.random.fold_in(key, 3), (N_DP,), 1, PMAX + 1)
    top_group = jax.random.randint(jax.random.fold_in(key, 7), (), 0, N_DP)
    page_limits = jnp.where(jnp.arange(N_DP, dtype=jnp.int32) == top_group, PMAX, page_limits)
    limits = (PAGE_LENGTH * page_limits)[:, None].astype(jnp.int32)
    drawn = jax.random.randint(jax.random.fold_in(key, 4), (N_DP, SEQ_DP), 2, limits + 1)
    peak_position = jax.random.randint(jax.random.fold_in(key, 8), (N_DP,), 0, SEQ_DP)
    at_peak = jnp.arange(SEQ_DP, dtype=jnp.int32)[None, :] == peak_position[:, None]
    drawn = jnp.where(at_peak, limits, drawn)
    return drawn.reshape(SEQUENCE_TOTAL).astype(jnp.int32)


def draw_queries(key, part):
    value_matrix = jax.random.truncated_normal(jax.random.fold_in(key, 5), -6.0, 6.0, (SEQUENCE_TOTAL, QUERY_HEADS * HEAD_WIDTH)).astype(jnp.float32)
    return value_matrix.astype(jnp.bfloat16)


def draw_page_cache(key, part):
    value_matrix = jax.random.truncated_normal(jax.random.fold_in(key, 6), -6.0, 6.0, (KEY_VALUE_HEADS, N_DP * N_MP * HOLDER_SLOTS, 2, PAGE_LENGTH, HEAD_WIDTH)).astype(jnp.float32)
    return value_matrix.astype(jnp.bfloat16)


def block_levels(stream_key, shape, shards, least, high):
    def one(axis_at, blocks):
        heights = jax.random.uniform(jax.random.fold_in(jax.random.fold_in(stream_key, 6), axis_at), (blocks,), jnp.float32, least / len(shards), high / len(shards))
        return jnp.repeat(jnp.exp(heights), shape[axis_at] // blocks).reshape((-1,) + (1,) * (len(shape) - axis_at - 1))

    gain = one(*shards[0])
    for cut in shards[1:]:
        gain = gain * one(*cut)
    return gain


def assign_block(rng, own, number, rows, count, top, bound, lean):
    order = jax.random.permutation(rng, count)
    packed, ordinary = shares(count, rows * top, bound, lean, True), shares(count, rows * top, bound, lean, False)
    places = jnp.arange(count)

    def named(sizes, turn):
        used = int((sizes > 0).sum())
        fixed = max(1, used // 4)
        shifted = fixed + (places - fixed + turn * (used - fixed)) % max(1, count - fixed)
        return jnp.zeros((count,), jnp.int32).at[order[jnp.where(places < fixed, places, shifted)]].set(jnp.asarray(sizes, jnp.int32))

    sizes = jnp.where(number % 4 == 0, named(packed, number // 4), named(ordinary, number - number // 4 - 1))
    mixed = jax.random.permutation(jax.random.fold_in(own, 3), count)
    donor, taker = mixed[0:count // 2 * 2:2], mixed[1:count // 2 * 2:2]
    margin = jnp.minimum(sizes[donor] - 1, bound - sizes[taker]) // 2
    margin = jnp.where((donor == order[0]) | (taker == order[0]) | (sizes[taker] == 0), 0, jnp.maximum(margin, 0))
    shifted = jax.random.randint(jax.random.fold_in(own, 4), (count // 2,), 0, 1 << 20) % (margin + 1)
    sizes = sizes.at[donor].add(-shifted).at[taker].add(shifted)
    members = jnp.searchsorted(jnp.cumsum(sizes), jnp.arange(rows * top), side="right").astype(jnp.int32)
    grid = members.reshape(top, rows).T
    grid = grid[jax.random.permutation(jax.random.fold_in(own, 1), rows)]
    turn = jax.random.randint(jax.random.fold_in(own, 2), (rows, 1), 0, top)
    return jnp.take_along_axis(grid, (jnp.arange(top)[None, :] + turn) % top, axis=1)


def shares(count, total, reach, lean, full):
    loads = [(1 << 20) // math.isqrt(rank ** lean) + 1 for rank in range(1, count + 1)]
    largest = reach if full else min(reach, max(-(-total // count), total * loads[0] // sum(loads)))
    least = 1 if total - largest >= count - 1 else 0
    counts, surplus = [largest] + [least] * (count - 1), total - largest - least * (count - 1)
    while surplus > 0:
        free = [i for i in range(1, count) if counts[i] < largest] or [i for i in range(1, count) if counts[i] < reach]
        whole, budget = sum([loads[i] for i in free]), surplus
        for i in free:
            extra = min(reach - counts[i], max(1, budget * loads[i] // whole), surplus)
            counts[i] = counts[i] + extra
            surplus = surplus - extra
    return np.array(counts)


def scatter_about(own_key, dims, spread, limit, cuts=(), kind=jnp.bfloat16):
    level = block_levels(own_key, dims, cuts, -0.22, 0.18) if cuts else 1.0
    result = jax.random.normal(own_key, dims, jnp.float32) * spread * level
    return jnp.minimum(jnp.maximum(result, -limit), limit).astype(kind)


def setup_inputs(seed: int = 0) -> dict:
    seeds = jax.random.split(jax.random.key(seed), 15)
    queries = draw_queries(jax.random.fold_in(seeds[14], 71), 0)
    fresh_entries = scatter_about(seeds[1], (2, SEQUENCE_TOTAL, KEY_VALUE_HEADS * HEAD_WIDTH), 1.0, 6.0, ((1, 8), (2, 8)))
    page_cache = draw_page_cache(jax.random.fold_in(seeds[14], 71), 0)
    lengths = draw_lengths(jax.random.fold_in(seeds[14], 71), 0)
    page_holder = draw_page_holder(jax.random.fold_in(seeds[14], 71), 0)
    page_slot = draw_page_slot(jax.random.fold_in(seeds[14], 71), 0)
    tokens = scatter_about(seeds[6], (SEQUENCE_TOTAL, D), 1.0, 6.0, ((0, 8),))
    norm_gain = jnp.clip(1.0 + 0.1 * jax.random.normal(seeds[7], (D,), jnp.float32), 0.5, 1.5)
    out_weight = scatter_about(seeds[8], (QUERY_HEADS * HEAD_WIDTH, D), (QUERY_HEADS * HEAD_WIDTH) ** -0.5, 0.09375, ((0, 32),))
    expert_ids_keys = jax.random.split(jax.random.fold_in(seeds[9], 1), SEQUENCE_TOTAL // SEQ_DP)
    expert_ids_turns = jax.random.permutation(jax.random.fold_in(seeds[9], 3), SEQUENCE_TOTAL // SEQ_DP)
    expert_ids = jax.vmap(lambda own, number: assign_block(jax.random.fold_in(seeds[9], 2), own, number, SEQ_DP, E, TOPK, CAP, 2))(expert_ids_keys, expert_ids_turns).reshape((SEQUENCE_TOTAL, TOPK))
    gate_values = jnp.clip(jax.random.uniform(seeds[10], (SEQUENCE_TOTAL, TOPK), jnp.float32, 0.1, 0.9), 0.1, 0.9)
    gate_weight = scatter_about(seeds[11], (E, D, FF), D ** -0.5, 0.09375, ((0, 8), (2, 32)))
    up_weight = scatter_about(seeds[12], (E, D, FF), D ** -0.5, 0.09375, ((0, 8), (2, 32)))
    down_weight = scatter_about(seeds[13], (E, FF, D), FF ** -0.5, 0.0625, ((0, 8), (1, 32)))
    return dict(queries=queries, fresh_entries=fresh_entries, page_cache=page_cache, lengths=lengths, page_holder=page_holder, page_slot=page_slot, tokens=tokens, norm_gain=norm_gain, out_weight=out_weight, expert_ids=expert_ids, gate_values=gate_values, gate_weight=gate_weight, up_weight=up_weight, down_weight=down_weight)


floor_score = -1e+30

def reference(queries, fresh_entries, page_cache, lengths, page_holder, page_slot, tokens, norm_gain, out_weight, expert_ids, gate_values, gate_weight, up_weight, down_weight):
    head_groups = QUERY_HEADS // KEY_VALUE_HEADS
    score_scale = HEAD_WIDTH ** (-0.5)
    key_extent = PAGE_LENGTH * PMAX
    highest_precision = lax.Precision.HIGHEST

    def attend_one(sequence_index):
        slot_rows = (page_holder[sequence_index] * HOLDER_SLOTS + page_slot[sequence_index]).astype(jnp.int32)
        page_contents = jnp.take(page_cache, slot_rows, axis=1).astype(jnp.float32)
        cached_key_rows = page_contents[:, :, 0].reshape(KEY_VALUE_HEADS, key_extent, HEAD_WIDTH)
        cached_value_rows = page_contents[:, :, 1].reshape(KEY_VALUE_HEADS, key_extent, HEAD_WIDTH)
        query_matrix = queries[sequence_index].astype(jnp.float32).reshape(KEY_VALUE_HEADS, head_groups, HEAD_WIDTH)
        fresh_key = fresh_entries[0, sequence_index].astype(jnp.float32).reshape(KEY_VALUE_HEADS, HEAD_WIDTH)
        fresh_value = fresh_entries[1, sequence_index].astype(jnp.float32).reshape(KEY_VALUE_HEADS, HEAD_WIDTH)
        scores = jnp.einsum('kgd,kpd->kgp', query_matrix, cached_key_rows, precision=highest_precision) * score_scale
        own_score = jnp.einsum('kgd,kd->kg', query_matrix, fresh_key, precision=highest_precision) * score_scale
        is_live = jnp.arange(key_extent, dtype=jnp.int32) < lengths[sequence_index]
        masked = jnp.where(is_live, scores, floor_score)
        highest = jnp.maximum(lax.optimization_barrier(jnp.max(masked, axis=2)), own_score)
        weights = jnp.where(is_live, jnp.exp(masked - highest[..., None]), 0.0)
        own_weight = jnp.exp(own_score - highest)
        totals = lax.optimization_barrier(jnp.sum(weights, axis=2)) + own_weight
        weighted = jnp.einsum('kgp,kpd->kgd', weights, cached_value_rows, precision=highest_precision)
        weighted = weighted + own_weight[..., None] * fresh_value[:, None, :]
        return (weighted / totals[..., None]).reshape(QUERY_HEADS * HEAD_WIDTH).astype(jnp.bfloat16)
    attended = lax.map(attend_one, jnp.arange(SEQUENCE_TOTAL, dtype=jnp.int32))
    residual = tokens.astype(jnp.float32) + jnp.dot(attended, out_weight, preferred_element_type=jnp.float32)
    normed = (residual * lax.rsqrt(lax.optimization_barrier(jnp.mean(residual * residual, axis=-1, keepdims=True)) + 1e-05) * norm_gain).astype(jnp.bfloat16)

    def expert_step(carry, expert):
        gate_out = jnp.dot(normed, gate_weight[expert], preferred_element_type=jnp.float32)
        up_out = jnp.dot(normed, up_weight[expert], preferred_element_type=jnp.float32)
        hidden = (jax.nn.silu(gate_out) * up_out).astype(jnp.bfloat16)
        projected = jnp.dot(hidden, down_weight[expert], preferred_element_type=jnp.float32)
        combine_weights = lax.optimization_barrier(jnp.sum(jnp.where(expert_ids == expert, gate_values, 0.0), axis=1))
        return (carry + combine_weights[:, None] * projected, None)
    moe, _ = lax.scan(expert_step, jnp.zeros((SEQUENCE_TOTAL, D), jnp.float32), jnp.arange(E, dtype=jnp.int32))
    return (residual + moe).astype(jnp.bfloat16)
```

```python
import functools

import jax
import jax.numpy as jnp
from jax import lax
from jax.experimental import pallas as pl
from jax.experimental.pallas import tpu as pltpu
from jax.sharding import Mesh, PartitionSpec as P

bf16 = jnp.bfloat16
f32 = jnp.float32
i32 = jnp.int32

DP, NX, NC, MP = 8, 4, 2, 4
EXPERTS = NX * NC
HOLDERS = DP * MP
PMAX = 4
SEQ = 32
TOTAL = DP * SEQ
SLOTS = 32
PAGE = 256
HEAD = 128
GROUPS = 4
D = 4096
FF = 256
CHIPS = NX * MP
COLS = D // CHIPS
HALF = SEQ // NC
ROWS = DP * HALF
FLOOR = -1e30
SCALE = HEAD ** (-0.5)


def iota(shape, dim):
    return lax.broadcasted_iota(i32, shape, dim)


def dot(a, b, dims=((1,), (0,))):
    return lax.dot_general(a, b, (dims, ((), ())), preferred_element_type=f32)


def one_hot(mask):
    return jnp.where(mask, 1.0, 0.0).astype(bf16)


def core_rows(core, count):
    row = iota((count, SEQ), 0)
    wanted = (row // MP) * (NC * MP) + core * MP + row % MP
    return one_hot(wanted == iota((count, SEQ), 1))


def select_kernel(place, queries, holders, out):
    lane = iota((GROUPS * SEQ, HEAD), 1)
    sub = iota((GROUPS * SEQ, HEAD), 0)
    table = jnp.concatenate([holders[...]] * GROUPS, axis=0)
    named = jnp.zeros((GROUPS * SEQ, HEAD), i32)
    for j in range(PMAX):
        named = jnp.where(lane % PMAX == j, table[:, j : j + 1], named)
    wanted = (lane // (GROUPS * PMAX)) * MP + place[3]
    same_head = (lane // PMAX) % GROUPS == sub // SEQ
    pick = one_hot((named == wanted) & same_head)
    stacked = jnp.concatenate(
        [queries[:, k * HEAD : (k + 1) * HEAD] for k in range(GROUPS)], axis=0
    )
    out[...] = dot(pick, stacked, ((0,), (0,))).astype(bf16)


def index_kernel(place, holders, slots, lengths, spread, live, gather):
    lane = iota((TOTAL, HEAD), 1)
    sub = iota((TOTAL, HEAD), 0)
    mine = place[0] * MP + place[3]
    named = jnp.zeros((TOTAL, HEAD), i32)
    slot = jnp.zeros((TOTAL, HEAD), i32)
    for j in range(PMAX):
        here = lane % PMAX == j
        named = jnp.where(here, holders[:, j : j + 1], named)
        slot = jnp.where(here, slots[:, j : j + 1], slot)
    keep = (named == mine) & (sub // SEQ == lane // (GROUPS * PMAX))
    slot_row = jnp.sum(jnp.where(keep, slot, 0), axis=0, keepdims=True)
    length_row = jnp.sum(jnp.where(keep, lengths[...], 0), axis=0, keepdims=True)
    one_lane = lane[0:1]
    live_row = jnp.clip(length_row - PAGE * (one_lane % PMAX), 0, PAGE)
    head_lane = (lane // PMAX) % GROUPS
    match = (slot_row == sub // 8) & (head_lane == sub % GROUPS)
    spread[...] = one_hot(match)
    count = jnp.sum(jnp.where(match, live_row, 0), axis=1, keepdims=True)
    live[...] = jnp.broadcast_to(count, (TOTAL, HEAD))
    own = (lane // (GROUPS * PMAX) == sub // SEQ) & (head_lane == (sub // 8) % GROUPS)
    own = own & (lane % PMAX == sub % PMAX)
    target = jnp.sum(jnp.where(own, slot_row, 0), axis=1, keepdims=True)
    rows = iota((TOTAL, 1), 0)
    target = target * 8 + (rows // 8) % GROUPS + jnp.where(rows % 8 < PMAX, 0, TOTAL)
    gather[...] = one_hot(target == iota((TOTAL, 2 * TOTAL), 1))


STEP = 8


def attend_kernel(queries, spread, live, gather, pages, out, parts):
    step = pl.program_id(0)
    wanted = dot(spread[...], queries[...])
    scores = jnp.concatenate(
        [
            dot(wanted[k * 8 : (k + 1) * 8].astype(bf16), pages[0, k, 0], ((1,), (1,)))
            for k in range(STEP)
        ],
        axis=0,
    )
    scores = scores * SCALE
    is_live = iota((STEP * 8, PAGE), 1) < live[:, 0:1]
    masked = jnp.where(is_live, scores, FLOOR)
    top = jnp.max(masked, axis=1, keepdims=True).astype(bf16).astype(f32)
    weights = jnp.where(is_live, jnp.exp(masked - top), 0.0)
    total = jnp.sum(weights, axis=1, keepdims=True)
    coarse = weights.astype(bf16).astype(f32)
    first = iota((STEP * 8, PAGE), 0) % 8 < GROUPS
    split = jnp.where(first, coarse, weights - coarse)
    found = []
    for k in range(STEP):
        both = dot(split[k * 8 : (k + 1) * 8].astype(bf16), pages[0, k, 1])
        found.append(both + pltpu.roll(both, GROUPS, 0))
    start = pl.multiple_of(step * (STEP * 8), STEP * 8)
    parts[pl.ds(start, STEP * 8), :] = jnp.concatenate(found, axis=0)
    lane = iota((STEP * 8, HEAD), 1)
    high = total.astype(bf16).astype(f32)
    tops = jnp.where(lane < 64, top, jnp.where(lane < 96, high, total - high))
    parts[pl.ds(TOTAL + start, STEP * 8), :] = tops

    @pl.when(step == SLOTS // STEP - 1)
    def _():
        out[...] = dot(gather[...], parts[...].astype(bf16)).astype(bf16)


PROJ = 4


def project_kernel(
    place, received, queries, fresh, holders, weight, mine, theirs, attended
):
    step = pl.program_id(0)

    @pl.when(step == 0)
    def _():
        table = holders[...]
        lane = iota((SEQ, TOTAL), 1)
        order = jnp.concatenate(
            [one_hot(table[:, r % PMAX : r % PMAX + 1] * 8 + r == lane) for r in range(8)],
            axis=0,
        )
        sorted_parts = dot(order, received[...])
        pages = [sorted_parts[j * SEQ : (j + 1) * SEQ] for j in range(PMAX)]
        scalars = [sorted_parts[(PMAX + j) * SEQ : (PMAX + j + 1) * SEQ] for j in range(PMAX)]
        own = (
            jnp.sum(
                queries[...].astype(f32) * fresh[0].astype(f32), axis=1, keepdims=True
            )
            * SCALE
        )
        highest = own
        for part in scalars:
            highest = jnp.maximum(highest, part[:, 0:1])
        factor = jnp.exp(own - highest)
        total = factor
        weighted = factor * fresh[1].astype(f32)
        for page, part in zip(pages, scalars):
            factor = jnp.exp(part[:, 0:1] - highest)
            total = total + (part[:, 64:65] + part[:, 96:97]) * factor
            weighted = weighted + page * factor
        rows = (weighted / total).astype(bf16)
        order = jnp.concatenate(
            [core_rows(place[2], HALF), core_rows(1 - place[2], HALF)], axis=0
        )
        attended[...] = dot(order, rows).astype(bf16)

    result = dot(attended[...], weight[...])
    for k in range(CHIPS // PROJ):
        block = result[:, k * COLS : (k + 1) * COLS]
        mine[k] = block[:HALF]
        theirs[k] = block[HALF:].astype(bf16)


def residual_kernel(place, received, tokens, gain, out):
    summed = jnp.sum(received[...].astype(f32), axis=0)
    own = dot(core_rows(place[2], HALF), tokens[...])
    gained = ((summed + own) * gain[...]).astype(bf16)
    out[...] = jnp.broadcast_to(gained[None], (DP, HALF, COLS))


def spread_kernel(rows, out):
    out[...] = jnp.broadcast_to(rows[...][None], out.shape)


UNITS = 4
BLOCKS = CHIPS // UNITS


def hidden_kernel(rows, gain, gate, up, routed, out, gate_sum, up_sum, squares):
    step = pl.program_id(0)

    @pl.when(step == 0)
    def _():
        gate_sum[...] = jnp.zeros_like(gate_sum)
        up_sum[...] = jnp.zeros_like(up_sum)
        squares[...] = jnp.zeros_like(squares)

    for k in range(BLOCKS):
        part = rows[k]
        weights = slice(k * COLS, (k + 1) * COLS)
        gate_sum[...] += dot(part, gate[0, weights])
        up_sum[...] += dot(part, up[0, weights])
        plain = part.astype(f32) / gain[:, weights]
        squares[...] += plain * plain

    @pl.when(step == UNITS - 1)
    def _():
        mean = jnp.sum(squares[...], axis=1, keepdims=True) * (1.0 / D)
        scale = lax.rsqrt(mean + 1e-05)
        gated = gate_sum[...] * scale
        value = gated / (1.0 + jnp.exp(-gated)) * (up_sum[...] * scale)
        value = (value * routed[...]).astype(bf16)
        row = iota((ROWS, ROWS), 0)
        order = one_hot((row % DP) * CHIPS + row // DP == iota((ROWS, ROWS), 1))
        out[...] = dot(order, value).astype(bf16)


def down_kernel(hidden, weight, out):
    out[...] = dot(hidden[...], weight[0]).astype(bf16)


def chip_sum_kernel(received, out):
    summed = jnp.sum(received[...].astype(f32), axis=0)
    out[...] = summed.reshape(DP, out.shape[1], HEAD).astype(bf16)


def final_kernel(received, residual, out):
    summed = jnp.sum(received[...].astype(f32), axis=0) + residual[...]
    for k in range(D // HEAD):
        out[:, k * HEAD : (k + 1) * HEAD] = summed[k : k + 1].astype(bf16)


def call(kernel, out_shape, grid, in_specs, out_specs, scratch=(), place=False, name=None):
    return pl.pallas_call(
        kernel,
        out_shape=out_shape,
        grid_spec=pltpu.PrefetchScalarGridSpec(
            num_scalar_prefetch=1 if place else 0,
            grid=grid,
            in_specs=in_specs,
            out_specs=out_specs,
            scratch_shapes=scratch,
        ),
        compiler_params=pltpu.CompilerParams(
            dimension_semantics=("arbitrary",) * len(grid)
        ),
        name=name,
    )


def whole(shape):
    return pl.BlockSpec(shape, lambda *_: (0,) * len(shape))


def struct(shape, dtype=bf16):
    return jax.ShapeDtypeStruct(shape, dtype)


def exchange(array, axes):
    return lax.all_to_all(array, axes, 0, 0, tiled=True)


def swap(array):
    return lax.ppermute(array, "core", [(0, 1), (1, 0)])


def body(
    queries,
    fresh_entries,
    page_cache,
    lengths,
    page_holder,
    page_slot,
    tokens,
    norm_gain,
    out_weight,
    expert_ids,
    gate_values,
    gate_weight,
    up_weight,
    down_weight,
):
    dp, x, core, mp = (lax.axis_index(n) for n in ("dp", "x", "core", "mp"))
    place = jnp.stack([dp, x, core, mp]).astype(i32)
    gain = norm_gain.reshape(1, D)

    selected = call(
        select_kernel,
        struct((DP * GROUPS * PMAX, HEAD)),
        (1,),
        [
            whole((SEQ, GROUPS * HEAD)),
            pl.BlockSpec((SEQ, PMAX), lambda _, p: (p[0], 0)),
        ],
        whole((DP * GROUPS * PMAX, HEAD)),
        place=True,
        name="select",
    )(place, queries, page_holder)
    asked = exchange(selected.reshape(DP, GROUPS * PMAX, HEAD), "dp")
    asked = asked.reshape(DP * GROUPS * PMAX, HEAD)

    spread, live, gather = call(
        index_kernel,
        (struct((TOTAL, HEAD)), struct((TOTAL, HEAD), i32), struct((TOTAL, 2 * TOTAL))),
        (1,),
        [whole((TOTAL, PMAX)), whole((TOTAL, PMAX)), whole((TOTAL, 1))],
        (whole((TOTAL, HEAD)), whole((TOTAL, HEAD)), whole((TOTAL, 2 * TOTAL))),
        place=True,
        name="index",
    )(place, page_holder, page_slot, lengths.reshape(TOTAL, 1))

    parts = call(
        attend_kernel,
        struct((TOTAL, HEAD)),
        (SLOTS // STEP,),
        [
            whole((DP * GROUPS * PMAX, HEAD)),
            pl.BlockSpec((STEP * 8, HEAD), lambda s: (s, 0)),
            pl.BlockSpec((STEP * 8, HEAD), lambda s: (s, 0)),
            whole((TOTAL, 2 * TOTAL)),
            pl.BlockSpec((1, STEP, 2, PAGE, HEAD), lambda s: (0, s, 0, 0, 0)),
        ],
        whole((TOTAL, HEAD)),
        scratch=[pltpu.VMEM((2 * TOTAL, HEAD), f32)],
        name="attend",
    )(asked, spread, live, gather, page_cache)
    parts = exchange(parts.reshape(HOLDERS, 8, HEAD), ("dp", "mp"))
    parts = parts.reshape(TOTAL, HEAD)

    mine, theirs = call(
        project_kernel,
        (struct((CHIPS, HALF, COLS), f32), struct((CHIPS, HALF, COLS))),
        (PROJ,),
        [
            whole((TOTAL, HEAD)),
            pl.BlockSpec((SEQ, HEAD), lambda _, p: (0, p[3])),
            whole((2, SEQ, HEAD)),
            pl.BlockSpec((SEQ, PMAX), lambda _, p: (p[0], 0)),
            pl.BlockSpec((HEAD, D // PROJ), lambda s, _: (0, s)),
        ],
        (
            pl.BlockSpec((CHIPS // PROJ, HALF, COLS), lambda s, _: (s, 0, 0)),
            pl.BlockSpec((CHIPS // PROJ, HALF, COLS), lambda s, _: (s, 0, 0)),
        ),
        scratch=[pltpu.VMEM((SEQ, HEAD), bf16)],
        place=True,
        name="project",
    )(place, parts, queries, fresh_entries, page_holder, out_weight)
    joined = (mine + swap(theirs).astype(f32)).astype(bf16)
    joined = exchange(joined, ("x", "mp"))

    gained = call(
        residual_kernel,
        struct((DP, HALF, COLS)),
        (1,),
        [
            whole((CHIPS, HALF, COLS)),
            pl.BlockSpec((SEQ, COLS), lambda _, p: (0, p[1] * MP + p[3])),
            pl.BlockSpec((1, COLS), lambda _, p: (0, p[1] * MP + p[3])),
        ],
        whole((DP, HALF, COLS)),
        place=True,
        name="residual",
    )(place, joined, tokens, gain)
    gained = exchange(gained, "dp").reshape(ROWS, COLS)
    copies = call(
        spread_kernel,
        struct((CHIPS, ROWS, COLS)),
        (1,),
        [whole((ROWS, COLS))],
        whole((CHIPS, ROWS, COLS)),
        name="spread",
    )(gained)
    own_rows = exchange(copies, ("x", "mp"))
    other_rows = swap(own_rows)

    expert = x * NC + core
    routed = jnp.sum(jnp.where(expert_ids == expert, gate_values, 0.0), axis=1)
    routed = routed.reshape(DP, NX, NC, MP).transpose(2, 0, 1, 3).reshape(NC, ROWS, 1)
    own_routed = lax.dynamic_index_in_dim(routed, core, 0, keepdims=False)
    other_routed = lax.dynamic_index_in_dim(routed, 1 - core, 0, keepdims=False)

    hidden = call(
        hidden_kernel,
        struct((ROWS, FF)),
        (UNITS,),
        [
            pl.BlockSpec((BLOCKS, ROWS, COLS), lambda s: (s, 0, 0)),
            pl.BlockSpec((1, D // UNITS), lambda s: (0, s)),
            pl.BlockSpec((1, D // UNITS, FF), lambda s: (0, s, 0)),
            pl.BlockSpec((1, D // UNITS, FF), lambda s: (0, s, 0)),
            whole((ROWS, 1)),
        ],
        whole((ROWS, FF)),
        scratch=[pltpu.VMEM((ROWS, FF), f32) for _ in range(3)],
        name="hidden",
    )
    down = call(
        down_kernel,
        struct((ROWS, D)),
        (4,),
        [whole((ROWS, FF)), pl.BlockSpec((1, FF, D // 4), lambda s: (0, 0, s))],
        pl.BlockSpec((ROWS, D // 4), lambda s: (0, s)),
        name="down",
    )
    own_hidden = hidden(own_rows, gain, gate_weight, up_weight, own_routed)
    other_hidden = hidden(other_rows, gain, gate_weight, up_weight, other_routed)
    other_out = down(other_hidden, down_weight)
    passed = swap(other_out)
    own_out = down(own_hidden, down_weight)
    summed = (own_out.astype(f32) + passed.astype(f32)).astype(bf16)
    summed = exchange(summed.reshape(CHIPS, DP, D), ("x", "mp"))
    rows = call(
        chip_sum_kernel,
        struct((DP, D // HEAD, HEAD)),
        (2,),
        [pl.BlockSpec((CHIPS, DP, D // 2), lambda s: (0, 0, s))],
        pl.BlockSpec((DP, D // HEAD // 2, HEAD), lambda s: (0, s, 0)),
        name="chip_sum",
    )(summed)
    rows = exchange(rows, "dp")

    home = dp * CHIPS + x * MP + mp
    residual = lax.dynamic_slice_in_dim(own_rows, home, 1, 1).reshape(1, D).astype(f32) / gain
    return call(
        final_kernel,
        struct((1, D)),
        (1,),
        [whole((DP, D // HEAD, HEAD)), whole((D // HEAD, HEAD))],
        whole((1, D)),
        name="final",
    )(rows, residual.reshape(D // HEAD, HEAD))


def solution(mesh):
    fine = Mesh(mesh.devices.reshape(DP, NX, NC, MP), ("dp", "x", "core", "mp"))
    expert = ("x", "core")
    return jax.shard_map(
        body,
        mesh=fine,
        in_specs=(
            P("dp", expert),
            P(None, "dp", expert),
            P(expert, ("dp", "mp"), None, None, None),
            P(),
            P(),
            P(),
            P("dp", None),
            P(),
            P((*expert, "mp"), None),
            P(),
            P(),
            P(expert, None, ("dp", "mp")),
            P(expert, None, ("dp", "mp")),
            P(expert, ("dp", "mp"), None),
        ),
        out_specs=P(("dp", *expert, "mp"), None),
        check_vma=False,
    )
```

```python
import jax
import jax.numpy as jnp
from jax import lax
from jax.experimental import pallas as pl
from jax.experimental.pallas import tpu as pltpu
from jax.sharding import Mesh, PartitionSpec as P

bf16 = jnp.bfloat16
f32 = jnp.float32
i32 = jnp.int32

DP, NX, NC, MP = 8, 4, 2, 4
EXPERTS = NX * NC
HOLDERS = DP * MP
PMAX = 4
SEQ = 32
TOTAL = DP * SEQ
SLOTS = 32
PAGE = 256
HEAD = 128
GROUPS = 4
D = 4096
FF = 256
CHIPS = NX * MP
COLS = D // CHIPS
HALF = SEQ // NC
ROWS = DP * HALF
FLOOR = -1e30
SCALE = HEAD ** (-0.5)


def iota(shape, dim):
    return lax.broadcasted_iota(i32, shape, dim)


def dot(a, b, dims=((1,), (0,))):
    return lax.dot_general(a, b, (dims, ((), ())), preferred_element_type=f32)


def one_hot(mask):
    return jnp.where(mask, 1.0, 0.0).astype(bf16)


def core_rows(core, count):
    row = iota((count, SEQ), 0)
    wanted = (row // MP) * (NC * MP) + core * MP + row % MP
    return one_hot(wanted == iota((count, SEQ), 1))


def select_kernel(queries, holders, out):
    first = lax.axis_index("dp") * SEQ
    table = pltpu.roll(holders[...], (TOTAL - first) % TOTAL, 1)[:, :SEQ]
    row = iota((HEAD, SEQ), 0)
    named = jnp.zeros((HEAD, SEQ), i32)
    for j in range(PMAX):
        named = jnp.where(row % PMAX == j, table[j : j + 1], named)
    wanted = (row // (GROUPS * PMAX)) * MP + lax.axis_index("mp")
    found = jnp.zeros((HEAD, HEAD), f32)
    for k in range(GROUPS):
        pick = one_hot((named == wanted) & ((row // PMAX) % GROUPS == k))
        found = found + dot(pick, queries[:, k * HEAD : (k + 1) * HEAD])
    out[...] = found.astype(bf16)


def index_kernel(holders, slots, lengths, pages, spread, live, gather, order):
    del pages
    mine = lax.axis_index("dp") * MP + lax.axis_index("mp")

    def rows_of(array, count):
        row = iota((count, TOTAL), 0)
        rows = jnp.zeros((count, TOTAL), i32)
        for j in range(PMAX):
            rows = jnp.where(row % PMAX == j, array[j : j + 1], rows)
        return rows

    def held(count, group):
        lane = iota((count, TOTAL), 1)
        return (rows_of(holders[...], count) == mine) & (lane // SEQ == group)

    def total(mask, values):
        return jnp.sum(jnp.where(mask, values, 0), axis=1, keepdims=True)

    row = iota((HEAD, TOTAL), 0)
    lane = iota((HEAD, TOTAL), 1)
    mask = held(HEAD, row // (GROUPS * PMAX))
    slot = total(mask, rows_of(slots[...], HEAD))
    length = total(mask, lengths[...])
    count = jnp.clip(length - PAGE * (iota((HEAD, 1), 0) % PMAX), 0, PAGE)
    match = (slot == lane // 8) & ((row // PMAX) % GROUPS == lane % GROUPS)
    turned = jnp.where(match, 1.0, 0.0).T.astype(bf16)
    spread[...] = turned
    live[...] = dot(turned, jnp.broadcast_to(count.astype(f32), (HEAD, HEAD)).astype(bf16))

    row = iota((TOTAL, TOTAL), 0)
    mask = held(TOTAL, row // SEQ)
    slot = total(mask, rows_of(slots[...], TOTAL))
    row = iota((TOTAL, 1), 0)
    target = slot * 8 + (row // 8) % GROUPS + jnp.where(row % 8 < PMAX, 0, TOTAL)
    gather[...] = one_hot(target == iota((TOTAL, 2 * TOTAL), 1))

    first = lax.axis_index("dp") * SEQ
    lane = iota((8, TOTAL), 1)
    named = jnp.zeros((8, TOTAL), i32)
    table = jnp.concatenate([holders[...]] * 2, axis=0)
    for r in range(8):
        rolled = pltpu.roll(table, (TOTAL - first + r * SEQ) % TOTAL, 1)
        named = jnp.where(lane // SEQ == r, rolled[r % PMAX : r % PMAX + 1], named)
    lane = iota((TOTAL, TOTAL), 1)
    match = named[0:1] * 8 + lane // SEQ == iota((TOTAL, TOTAL), 0)
    order[...] = jnp.where(match, 1.0, 0.0).T.astype(bf16)


STEP = 8


def attend_kernel(queries, spread, live, gather, pages, out, parts):
    for step in range(SLOTS // STEP):
        rows = slice(step * STEP * 8, (step + 1) * STEP * 8)
        wanted = dot(spread[rows], queries[...])
        scores = jnp.concatenate(
            [
                dot(
                    wanted[k * 8 : (k + 1) * 8].astype(bf16),
                    pages[0, step * STEP + k, 0],
                    ((1,), (1,)),
                )
                for k in range(STEP)
            ],
            axis=0,
        )
        scores = scores * SCALE
        position = iota((STEP * 8, PAGE), 1).astype(f32)
        is_live = position < live[rows, 0:1]
        masked = jnp.where(is_live, scores, FLOOR)
        top = jnp.max(masked, axis=1, keepdims=True).astype(bf16).astype(f32)
        weights = jnp.where(is_live, jnp.exp(masked - top), 0.0)
        total = jnp.sum(weights, axis=1, keepdims=True)
        coarse = weights.astype(bf16).astype(f32)
        first = iota((STEP * 8, PAGE), 0) % 8 < GROUPS
        split = jnp.where(first, coarse, weights - coarse)
        found = []
        for k in range(STEP):
            both = dot(split[k * 8 : (k + 1) * 8].astype(bf16), pages[0, step * STEP + k, 1])
            found.append(both + pltpu.roll(both, GROUPS, 0))
        parts[rows, :] = jnp.concatenate(found, axis=0)
        lane = iota((STEP * 8, HEAD), 1)
        high = total.astype(bf16).astype(f32)
        tops = jnp.where(lane < 64, top, jnp.where(lane < 96, high, total - high))
        parts[TOTAL + step * STEP * 8 : TOTAL + (step + 1) * STEP * 8, :] = tops
    out[...] = dot(gather[...], parts[...].astype(bf16)).astype(bf16)


PROJ = 4


def project_kernel(received, queries, fresh, order, weight, mine, theirs):
    core = lax.axis_index("core")
    head = pl.multiple_of(lax.axis_index("mp") * HEAD, HEAD)
    sorted_parts = dot(order[...], received[...])
    pages = [sorted_parts[j * SEQ : (j + 1) * SEQ] for j in range(PMAX)]
    scalars = [sorted_parts[(PMAX + j) * SEQ : (PMAX + j + 1) * SEQ] for j in range(PMAX)]
    asked = queries[:, pl.ds(head, HEAD)].astype(f32)
    own = jnp.sum(asked * fresh[0].astype(f32), axis=1, keepdims=True) * SCALE
    highest = own
    for part in scalars:
        highest = jnp.maximum(highest, part[:, 0:1])
    factor = jnp.exp(own - highest)
    total = factor
    weighted = factor * fresh[1].astype(f32)
    for page, part in zip(pages, scalars):
        factor = jnp.exp(part[:, 0:1] - highest)
        total = total + (part[:, 64:65] + part[:, 96:97]) * factor
        weighted = weighted + page * factor
    rows = (weighted / total).astype(bf16)
    both = jnp.concatenate([core_rows(core, HALF), core_rows(1 - core, HALF)], axis=0)
    attended = dot(both, rows).astype(bf16)
    for k in range(CHIPS):
        block = dot(attended, weight[:, k * COLS : (k + 1) * COLS])
        mine[k] = block[:HALF]
        theirs[k] = block[HALF:].astype(bf16)


def join_kernel(mine, theirs, out):
    out[...] = (mine[...].astype(f32) + theirs[...].astype(f32)).astype(bf16)


def residual_kernel(received, tokens, gain, out):
    chip = lax.axis_index("x") * MP + lax.axis_index("mp")
    cols = pl.ds(pl.multiple_of(chip * COLS, COLS), COLS)
    summed = jnp.sum(received[...].astype(f32), axis=0)
    own = dot(core_rows(lax.axis_index("core"), HALF), tokens[:, cols])
    gained = ((summed + own) * gain[:, cols]).astype(bf16)
    out[...] = jnp.broadcast_to(gained[None], (DP, HALF, COLS))


def spread_kernel(rows, out):
    out[...] = jnp.broadcast_to(rows[...][None], out.shape)


def hidden_of(rows, gain, gate, up, ids, values, core):
    part = jnp.concatenate([rows[k] for k in range(CHIPS)], axis=1)
    gate_sum = dot(part, gate[0])
    up_sum = dot(part, up[0])
    inverse = 1.0 / gain[...]
    squares = jnp.zeros((ROWS, COLS), f32)
    for k in range(CHIPS):
        plain = rows[k].astype(f32) * inverse[:, k * COLS : (k + 1) * COLS]
        squares = squares + plain * plain
    mean = jnp.sum(squares, axis=1, keepdims=True) * (1.0 / D)
    scale = lax.rsqrt(mean + 1e-05)
    gated = gate_sum * scale
    value = gated / (1.0 + jnp.exp(-gated)) * (up_sum * scale)
    expert = lax.axis_index("x") * NC + lax.axis_index("core")
    routed = jnp.sum(jnp.where(ids[...] == expert, values[...], 0.0), axis=0, keepdims=True)
    row = iota((ROWS, TOTAL), 0)
    token = (row // CHIPS) * SEQ + ((row % CHIPS) // MP) * (NC * MP) + core * MP + row % MP
    picked = jnp.where(token == iota((ROWS, TOTAL), 1), routed, 0.0)
    value = (value * jnp.sum(picked, axis=1, keepdims=True)).astype(bf16)
    row = iota((ROWS, ROWS), 0)
    order = one_hot((row % DP) * CHIPS + row // DP == iota((ROWS, ROWS), 1))
    return dot(order, value).astype(bf16)


def own_kernel(rows, gain, gate, up, ids, values, out, residual):
    out[...] = hidden_of(rows, gain, gate, up, ids, values, lax.axis_index("core"))
    home = lax.axis_index("dp") * CHIPS + lax.axis_index("x") * MP + lax.axis_index("mp")
    pick = one_hot(iota((8, ROWS), 1) == home)
    for k in range(CHIPS):
        row = dot(pick, rows[k])
        residual[2 * k : 2 * k + 1] = row[:1, :HEAD]
        residual[2 * k + 1 : 2 * k + 2] = row[:1, HEAD:]


def other_kernel(after, rows, gain, gate, up, ids, values, weight, out):
    del after
    hidden = hidden_of(rows, gain, gate, up, ids, values, 1 - lax.axis_index("core"))
    for k in range(CHIPS):
        cols = slice(k * COLS, (k + 1) * COLS)
        out[:, cols] = dot(hidden, weight[0, :, cols]).astype(bf16)


def down_kernel(hidden, weight, out):
    for k in range(CHIPS):
        cols = slice(k * COLS, (k + 1) * COLS)
        out[:, cols] = dot(hidden[...], weight[0, :, cols]).astype(bf16)


def chip_sum_kernel(received, out):
    for k in range(CHIPS):
        cols = slice(k * COLS, (k + 1) * COLS)
        summed = jnp.sum(received[:, :, cols].astype(f32), axis=0)
        out[:, 2 * k : 2 * k + 2, :] = summed.reshape(DP, 2, HEAD).astype(bf16)


def final_kernel(received, residual, gain, out):
    summed = jnp.sum(received[...].astype(f32), axis=0) + residual[...] / gain[...]
    for k in range(D // HEAD):
        out[:, k * HEAD : (k + 1) * HEAD] = summed[k : k + 1].astype(bf16)


def call(kernel, out_shape, arrays, scratch=(), limit=8, name=None):
    vmem = pl.BlockSpec(memory_space=pltpu.VMEM)
    return pl.pallas_call(
        kernel,
        out_shape=out_shape,
        in_specs=[vmem] * len(arrays),
        out_specs=jax.tree.map(lambda _: vmem, out_shape),
        scratch_shapes=scratch,
        compiler_params=pltpu.CompilerParams(vmem_limit_bytes=limit * 2**20),
        name=name,
    )(*arrays)


def struct(shape, dtype=bf16):
    return jax.ShapeDtypeStruct(shape, dtype)


def exchange(array, axes):
    return lax.all_to_all(array, axes, 0, 0, tiled=True)


def swap(array):
    return lax.ppermute(array, "core", [(0, 1), (1, 0)])


def body(
    queries,
    fresh_entries,
    page_cache,
    lengths,
    page_holder,
    page_slot,
    tokens,
    norm_gain,
    out_weight,
    expert_ids,
    gate_values,
    gate_weight,
    up_weight,
    down_weight,
):
    gain = norm_gain.reshape(1, D)
    holders = page_holder.T
    ids = expert_ids.T
    values = gate_values.T

    lines = DP * GROUPS * PMAX
    selected = call(select_kernel, struct((lines, HEAD)), (queries, holders), name="select")
    asked = exchange(selected.reshape(DP, GROUPS * PMAX, HEAD), "dp").reshape(lines, HEAD)
    spread, live, gather, order = call(
        index_kernel,
        (
            struct((TOTAL, HEAD)),
            struct((TOTAL, HEAD), f32),
            struct((TOTAL, 2 * TOTAL)),
            struct((TOTAL, TOTAL)),
        ),
        (holders, page_slot.T, lengths.reshape(1, TOTAL), page_cache),
        name="index",
    )
    parts = call(
        attend_kernel,
        struct((TOTAL, HEAD)),
        (asked, spread, live, gather, page_cache),
        scratch=[pltpu.VMEM((2 * TOTAL, HEAD), f32)],
        name="attend",
    )
    parts = exchange(parts.reshape(HOLDERS, 8, HEAD), ("dp", "mp")).reshape(TOTAL, HEAD)

    mine, theirs = call(
        project_kernel,
        (struct((CHIPS, HALF, COLS), f32), struct((CHIPS, HALF, COLS))),
        (parts, queries, fresh_entries, order, out_weight),
        name="project",
    )
    joined = call(
        join_kernel, struct((CHIPS, HALF, COLS)), (mine, swap(theirs)), name="join_heads"
    )
    joined = exchange(joined, ("x", "mp"))

    gained = call(
        residual_kernel, struct((DP, HALF, COLS)), (joined, tokens, gain), name="residual"
    )
    gained = exchange(gained, "dp").reshape(ROWS, COLS)
    copies = call(spread_kernel, struct((CHIPS, ROWS, COLS)), (gained,), name="spread")
    own_rows = exchange(copies, ("x", "mp"))
    other_rows = swap(own_rows)

    own_hidden, residual = call(
        own_kernel,
        (struct((ROWS, FF)), struct((D // HEAD, HEAD), f32)),
        (own_rows, gain, gate_weight, up_weight, ids, values),
        name="own",
    )
    other_out = call(
        other_kernel,
        struct((ROWS, D)),
        (own_hidden, other_rows, gain, gate_weight, up_weight, ids, values, down_weight),
        name="other",
    )
    passed = swap(other_out)
    own_out = call(down_kernel, struct((ROWS, D)), (own_hidden, down_weight), name="down")
    summed = call(join_kernel, struct((ROWS, D)), (own_out, passed), name="join_experts")
    summed = exchange(summed.reshape(CHIPS, DP, D), ("x", "mp"))
    rows = call(chip_sum_kernel, struct((DP, D // HEAD, HEAD)), (summed,), name="chip_sum")
    rows = exchange(rows, "dp")
    return call(
        final_kernel,
        struct((1, D)),
        (rows, residual, norm_gain.reshape(D // HEAD, HEAD)),
        name="final",
    )


def solution(mesh):
    fine = Mesh(mesh.devices.reshape(DP, NX, NC, MP), ("dp", "x", "core", "mp"))
    expert = ("x", "core")
    return jax.shard_map(
        body,
        mesh=fine,
        in_specs=(
            P("dp", expert),
            P(None, "dp", expert),
            P(expert, ("dp", "mp"), None, None, None),
            P(),
            P(),
            P(),
            P("dp", None),
            P(),
            P((*expert, "mp"), None),
            P(),
            P(),
            P(expert, None, ("dp", "mp")),
            P(expert, None, ("dp", "mp")),
            P(expert, ("dp", "mp"), None),
        ),
        out_specs=P(("dp", *expert, "mp"), None),
        check_vma=False,
    )
```

```python
import jax
import jax.numpy as jnp
from jax import lax
from jax.experimental import pallas as pl
from jax.experimental.pallas import tpu as pltpu
from jax.sharding import Mesh, PartitionSpec as P

bf16 = jnp.bfloat16
f32 = jnp.float32
i32 = jnp.int32

DP, NX, NC, MP = 8, 4, 2, 4
EXPERTS = NX * NC
HOLDERS = DP * MP
PMAX = 4
SEQ = 32
TOTAL = DP * SEQ
SLOTS = 32
PAGE = 256
HEAD = 128
GROUPS = 4
D = 4096
FF = 256
CHIPS = NX * MP
COLS = D // CHIPS
HALF = SEQ // NC
ROWS = DP * HALF
FLOOR = -1e30
SCALE = HEAD ** (-0.5)


def iota(shape, dim):
    return lax.broadcasted_iota(i32, shape, dim)


def dot(a, b, dims=((1,), (0,))):
    return lax.dot_general(a, b, (dims, ((), ())), preferred_element_type=f32)


def one_hot(mask):
    return jnp.where(mask, 1.0, 0.0).astype(bf16)


def core_rows(core, count):
    row = iota((count, SEQ), 0)
    wanted = (row // MP) * (NC * MP) + core * MP + row % MP
    return one_hot(wanted == iota((count, SEQ), 1))


def select(queries, holders, out):
    first = lax.axis_index("dp") * SEQ
    table = pltpu.roll(holders[...], (TOTAL - first) % TOTAL, 1)[:, :SEQ]
    row = iota((HEAD, SEQ), 0)
    named = jnp.zeros((HEAD, SEQ), i32)
    for j in range(PMAX):
        named = jnp.where(row % PMAX == j, table[j : j + 1], named)
    wanted = (row // (GROUPS * PMAX)) * MP + lax.axis_index("mp")
    found = jnp.zeros((HEAD, HEAD), f32)
    for k in range(GROUPS):
        pick = one_hot((named == wanted) & ((row // PMAX) % GROUPS == k))
        found = found + dot(pick, queries[:, k * HEAD : (k + 1) * HEAD])
    out[...] = found.astype(bf16)


def select_kernel(queries, holders, slots, lengths, out, spread, live, gather, order):
    select(queries, holders, out)
    mine = lax.axis_index("dp") * MP + lax.axis_index("mp")

    def rows_of(array, count):
        row = iota((count, TOTAL), 0)
        rows = jnp.zeros((count, TOTAL), i32)
        for j in range(PMAX):
            rows = jnp.where(row % PMAX == j, array[j : j + 1], rows)
        return rows

    def held(count, group):
        lane = iota((count, TOTAL), 1)
        return (rows_of(holders[...], count) == mine) & (lane // SEQ == group)

    def total(mask, values):
        return jnp.sum(jnp.where(mask, values, 0), axis=1, keepdims=True)

    row = iota((HEAD, TOTAL), 0)
    lane = iota((HEAD, TOTAL), 1)
    mask = held(HEAD, row // (GROUPS * PMAX))
    slot = total(mask, rows_of(slots[...], HEAD))
    length = total(mask, lengths[...])
    count = jnp.clip(length - PAGE * (iota((HEAD, 1), 0) % PMAX), 0, PAGE)
    match = (slot == lane // 8) & ((row // PMAX) % GROUPS == lane % GROUPS)
    turned = jnp.where(match, 1.0, 0.0).T.astype(bf16)
    spread[...] = turned
    live[...] = dot(turned, jnp.broadcast_to(count.astype(f32), (HEAD, HEAD)).astype(bf16))

    row = iota((TOTAL, TOTAL), 0)
    mask = held(TOTAL, row // SEQ)
    slot = total(mask, rows_of(slots[...], TOTAL))
    row = iota((TOTAL, 1), 0)
    target = slot * 8 + (row // 8) % GROUPS + jnp.where(row % 8 < PMAX, 0, TOTAL)
    gather[...] = one_hot(target == iota((TOTAL, 2 * TOTAL), 1))

    first = lax.axis_index("dp") * SEQ
    lane = iota((8, TOTAL), 1)
    named = jnp.zeros((8, TOTAL), i32)
    table = jnp.concatenate([holders[...]] * 2, axis=0)
    for r in range(8):
        rolled = pltpu.roll(table, (TOTAL - first + r * SEQ) % TOTAL, 1)
        named = jnp.where(lane // SEQ == r, rolled[r % PMAX : r % PMAX + 1], named)
    lane = iota((TOTAL, TOTAL), 1)
    match = named[0:1] * 8 + lane // SEQ == iota((TOTAL, TOTAL), 0)
    order[...] = jnp.where(match, 1.0, 0.0).T.astype(bf16)


STEP = 8


def attend_kernel(queries, spread, live, gather, pages, out, parts):
    for step in range(SLOTS // STEP):
        rows = slice(step * STEP * 8, (step + 1) * STEP * 8)
        wanted = dot(spread[rows], queries[...])
        scores = jnp.concatenate(
            [
                dot(
                    wanted[k * 8 : (k + 1) * 8].astype(bf16),
                    pages[0, step * STEP + k, 0],
                    ((1,), (1,)),
                )
                for k in range(STEP)
            ],
            axis=0,
        )
        scores = scores * SCALE
        position = iota((STEP * 8, PAGE), 1).astype(f32)
        is_live = position < live[rows, 0:1]
        masked = jnp.where(is_live, scores, FLOOR)
        top = jnp.max(masked, axis=1, keepdims=True).astype(bf16).astype(f32)
        weights = jnp.where(is_live, jnp.exp(masked - top), 0.0)
        total = jnp.sum(weights, axis=1, keepdims=True)
        coarse = weights.astype(bf16).astype(f32)
        first = iota((STEP * 8, PAGE), 0) % 8 < GROUPS
        split = jnp.where(first, coarse, weights - coarse)
        found = []
        for k in range(STEP):
            both = dot(split[k * 8 : (k + 1) * 8].astype(bf16), pages[0, step * STEP + k, 1])
            found.append(both + pltpu.roll(both, GROUPS, 0))
        parts[rows, :] = jnp.concatenate(found, axis=0)
        lane = iota((STEP * 8, HEAD), 1)
        high = total.astype(bf16).astype(f32)
        tops = jnp.where(lane < 64, top, jnp.where(lane < 96, high, total - high))
        parts[TOTAL + step * STEP * 8 : TOTAL + (step + 1) * STEP * 8, :] = tops
    out[...] = dot(gather[...], parts[...].astype(bf16)).astype(bf16)


PROJ = 4


def project_kernel(received, queries, fresh, order, weight, mine, theirs):
    core = lax.axis_index("core")
    head = pl.multiple_of(lax.axis_index("mp") * HEAD, HEAD)
    sorted_parts = dot(order[...], received[...])
    pages = [sorted_parts[j * SEQ : (j + 1) * SEQ] for j in range(PMAX)]
    scalars = [sorted_parts[(PMAX + j) * SEQ : (PMAX + j + 1) * SEQ] for j in range(PMAX)]
    asked = queries[:, pl.ds(head, HEAD)].astype(f32)
    own = jnp.sum(asked * fresh[0].astype(f32), axis=1, keepdims=True) * SCALE
    highest = own
    for part in scalars:
        highest = jnp.maximum(highest, part[:, 0:1])
    factor = jnp.exp(own - highest)
    total = factor
    weighted = factor * fresh[1].astype(f32)
    for page, part in zip(pages, scalars):
        factor = jnp.exp(part[:, 0:1] - highest)
        total = total + (part[:, 64:65] + part[:, 96:97]) * factor
        weighted = weighted + page * factor
    rows = (weighted / total).astype(bf16)
    both = jnp.concatenate([core_rows(core, HALF), core_rows(1 - core, HALF)], axis=0)
    attended = dot(both, rows).astype(bf16)
    for k in range(CHIPS):
        block = dot(attended, weight[:, k * COLS : (k + 1) * COLS])
        mine[k] = block[:HALF]
        theirs[k] = block[HALF:].astype(bf16)


def join_kernel(mine, theirs, out):
    out[...] = (mine[...].astype(f32) + theirs[...].astype(f32)).astype(bf16)


def residual_kernel(received, tokens, gain, out):
    chip = lax.axis_index("x") * MP + lax.axis_index("mp")
    cols = pl.ds(pl.multiple_of(chip * COLS, COLS), COLS)
    summed = jnp.sum(received[...].astype(f32), axis=0)
    own = dot(core_rows(lax.axis_index("core"), HALF), tokens[:, cols])
    gained = ((summed + own) * gain[:, cols]).astype(bf16)
    out[...] = jnp.broadcast_to(gained[None], (DP, HALF, COLS))


def spread_kernel(rows, out):
    out[...] = jnp.broadcast_to(rows[...][None], out.shape)


def hidden_of(rows, gain, gate, up, ids, values, core):
    part = jnp.concatenate([rows[k] for k in range(CHIPS)], axis=1)
    gate_sum = dot(part, gate[0])
    up_sum = dot(part, up[0])
    inverse = 1.0 / gain[...]
    squares = jnp.zeros((ROWS, COLS), f32)
    for k in range(CHIPS):
        plain = rows[k].astype(f32) * inverse[:, k * COLS : (k + 1) * COLS]
        squares = squares + plain * plain
    mean = jnp.sum(squares, axis=1, keepdims=True) * (1.0 / D)
    scale = lax.rsqrt(mean + 1e-05)
    gated = gate_sum * scale
    value = gated / (1.0 + jnp.exp(-gated)) * (up_sum * scale)
    expert = lax.axis_index("x") * NC + lax.axis_index("core")
    routed = jnp.sum(jnp.where(ids[...] == expert, values[...], 0.0), axis=0, keepdims=True)
    row = iota((ROWS, TOTAL), 0)
    token = (row // CHIPS) * SEQ + ((row % CHIPS) // MP) * (NC * MP) + core * MP + row % MP
    picked = jnp.where(token == iota((ROWS, TOTAL), 1), routed, 0.0)
    value = (value * jnp.sum(picked, axis=1, keepdims=True)).astype(bf16)
    row = iota((ROWS, ROWS), 0)
    order = one_hot((row % DP) * CHIPS + row // DP == iota((ROWS, ROWS), 1))
    return dot(order, value).astype(bf16)


def own_kernel(rows, gain, gate, up, ids, values, out, residual):
    out[...] = hidden_of(rows, gain, gate, up, ids, values, lax.axis_index("core"))
    home = lax.axis_index("dp") * CHIPS + lax.axis_index("x") * MP + lax.axis_index("mp")
    pick = one_hot(iota((8, ROWS), 1) == home)
    for k in range(CHIPS):
        row = dot(pick, rows[k])
        residual[2 * k : 2 * k + 1] = row[:1, :HEAD]
        residual[2 * k + 1 : 2 * k + 2] = row[:1, HEAD:]


def other_kernel(after, rows, gain, gate, up, ids, values, weight, out):
    del after
    hidden = hidden_of(rows, gain, gate, up, ids, values, 1 - lax.axis_index("core"))
    for k in range(CHIPS):
        cols = slice(k * COLS, (k + 1) * COLS)
        block = dot(hidden, weight[0, :, cols]).reshape(CHIPS, DP, COLS)
        out[:, k * DP : (k + 1) * DP, :] = block.astype(bf16)


def down_kernel(hidden, weight, out):
    for k in range(CHIPS):
        cols = slice(k * COLS, (k + 1) * COLS)
        block = dot(hidden[...], weight[0, :, cols]).reshape(CHIPS, DP, COLS)
        out[:, k * DP : (k + 1) * DP, :] = block.astype(bf16)


def chip_sum_kernel(received, out):
    for k in range(CHIPS):
        summed = jnp.sum(received[:, k * DP : (k + 1) * DP, :].astype(f32), axis=0)
        out[:, 2 * k : 2 * k + 2, :] = summed.reshape(DP, 2, HEAD).astype(bf16)


def final_kernel(received, residual, gain, out):
    summed = jnp.sum(received[...].astype(f32), axis=0) + residual[...] / gain[...]
    for k in range(D // HEAD):
        out[:, k * HEAD : (k + 1) * HEAD] = summed[k : k + 1].astype(bf16)


def call(kernel, out_shape, arrays, scratch=(), limit=8, micros=0, name=None):
    vmem = pl.BlockSpec(memory_space=pltpu.VMEM)
    return pl.pallas_call(
        kernel,
        out_shape=out_shape,
        in_specs=[vmem] * len(arrays),
        out_specs=jax.tree.map(lambda _: vmem, out_shape),
        scratch_shapes=scratch,
        compiler_params=pltpu.CompilerParams(vmem_limit_bytes=limit * 2**20),
        cost_estimate=pl.CostEstimate(
            flops=micros * 10**8, bytes_accessed=micros * 10**6, transcendentals=0
        )
        if micros
        else None,
        name=name,
    )(*arrays)


def struct(shape, dtype=bf16):
    return jax.ShapeDtypeStruct(shape, dtype)


def exchange(array, axes):
    return lax.all_to_all(array, axes, 0, 0, tiled=True)


def swap(array):
    return lax.ppermute(array, "core", [(0, 1), (1, 0)])


def body(
    queries,
    fresh_entries,
    page_cache,
    lengths,
    page_holder,
    page_slot,
    tokens,
    norm_gain,
    out_weight,
    expert_ids,
    gate_values,
    gate_weight,
    up_weight,
    down_weight,
):
    gain = norm_gain.reshape(1, D)
    holders = page_holder.T
    ids = expert_ids.T
    values = gate_values.T

    lines = DP * GROUPS * PMAX
    selected, spread, live, gather, order = call(
        select_kernel,
        (
            struct((lines, HEAD)),
            struct((TOTAL, HEAD)),
            struct((TOTAL, HEAD), f32),
            struct((TOTAL, 2 * TOTAL)),
            struct((TOTAL, TOTAL)),
        ),
        tuple(
            pltpu.with_memory_space_constraint(array, pltpu.HBM)
            for array in (queries, holders, page_slot.T, lengths.reshape(1, TOTAL))
        ),
        micros=8,
        name="select",
    )
    asked = exchange(selected.reshape(DP, GROUPS * PMAX, HEAD), "dp").reshape(lines, HEAD)
    parts = call(
        attend_kernel,
        struct((TOTAL, HEAD)),
        (asked, spread, live, gather, page_cache),
        scratch=[pltpu.VMEM((2 * TOTAL, HEAD), f32)],
        name="attend",
    )
    parts = exchange(parts.reshape(HOLDERS, 8, HEAD), ("dp", "mp")).reshape(TOTAL, HEAD)

    mine, theirs = call(
        project_kernel,
        (struct((CHIPS, HALF, COLS), f32), struct((CHIPS, HALF, COLS))),
        (parts, queries, fresh_entries, order, out_weight),
        name="project",
    )
    joined = call(
        join_kernel, struct((CHIPS, HALF, COLS)), (mine, swap(theirs)), name="join_heads"
    )
    joined = exchange(joined, ("x", "mp"))

    gained = call(
        residual_kernel, struct((DP, HALF, COLS)), (joined, tokens, gain), name="residual"
    )
    gained = exchange(gained, "dp").reshape(ROWS, COLS)
    copies = call(spread_kernel, struct((CHIPS, ROWS, COLS)), (gained,), name="spread")
    own_rows = exchange(copies, ("x", "mp"))
    other_rows = swap(own_rows)

    own_hidden, residual = call(
        own_kernel,
        (struct((ROWS, FF)), struct((D // HEAD, HEAD), f32)),
        (own_rows, gain, gate_weight, up_weight, ids, values),
        name="own",
    )
    other_out = call(
        other_kernel,
        struct((CHIPS, ROWS, COLS)),
        (own_hidden, other_rows, gain, gate_weight, up_weight, ids, values, down_weight),
        name="other",
    )
    passed = swap(other_out)
    own_out = call(down_kernel, struct((CHIPS, ROWS, COLS)), (own_hidden, down_weight), name="down")
    summed = call(
        join_kernel, struct((CHIPS, ROWS, COLS)), (own_out, passed), name="join_experts"
    )
    summed = exchange(summed, ("x", "mp"))
    rows = call(chip_sum_kernel, struct((DP, D // HEAD, HEAD)), (summed,), name="chip_sum")
    rows = exchange(rows, "dp")
    return call(
        final_kernel,
        struct((1, D)),
        (rows, residual, norm_gain.reshape(D // HEAD, HEAD)),
        name="final",
    )


def solution(mesh):
    fine = Mesh(mesh.devices.reshape(DP, NX, NC, MP), ("dp", "x", "core", "mp"))
    expert = ("x", "core")
    return jax.shard_map(
        body,
        mesh=fine,
        in_specs=(
            P("dp", expert),
            P(None, "dp", expert),
            P(expert, ("dp", "mp"), None, None, None),
            P(),
            P(),
            P(),
            P("dp", None),
            P(),
            P((*expert, "mp"), None),
            P(),
            P(),
            P(expert, None, ("dp", "mp")),
            P(expert, None, ("dp", "mp")),
            P(expert, ("dp", "mp"), None),
        ),
        out_specs=P(("dp", *expert, "mp"), None),
        check_vma=False,
    )
```

```python
import jax
import jax.numpy as jnp
from jax import lax
from jax.experimental import pallas as pl
from jax.experimental.pallas import tpu as pltpu
from jax.sharding import Mesh, PartitionSpec as P

bf16 = jnp.bfloat16
f32 = jnp.float32
i32 = jnp.int32

DP, NX, NC, MP = 8, 4, 2, 4
EXPERTS = NX * NC
HOLDERS = DP * MP
PMAX = 4
SEQ = 32
TOTAL = DP * SEQ
SLOTS = 32
PAGE = 256
HEAD = 128
GROUPS = 4
D = 4096
FF = 256
CAP = 16
CHIPS = NX * MP
COLS = D // CHIPS
HALF = SEQ // NC
ROWS = DP * HALF
FLOOR = -1e30
SCALE = HEAD ** (-0.5)


def iota(shape, dim):
    return lax.broadcasted_iota(i32, shape, dim)


def dot(a, b, dims=((1,), (0,))):
    return lax.dot_general(a, b, (dims, ((), ())), preferred_element_type=f32)


def one_hot(mask):
    return jnp.where(mask, 1.0, 0.0).astype(bf16)


def select_kernel(queries, holders, out):
    first = lax.axis_index("dp") * SEQ
    table = pltpu.roll(holders[...], (TOTAL - first) % TOTAL, 1)[:, :SEQ]
    row = iota((HEAD, SEQ), 0)
    named = jnp.zeros((HEAD, SEQ), i32)
    for j in range(PMAX):
        named = jnp.where(row % PMAX == j, table[j : j + 1], named)
    wanted = (row // (GROUPS * PMAX)) * MP + lax.axis_index("mp")
    found = jnp.zeros((HEAD, HEAD), f32)
    for k in range(GROUPS):
        pick = one_hot((named == wanted) & ((row // PMAX) % GROUPS == k))
        found = found + dot(pick, queries[:, k * HEAD : (k + 1) * HEAD])
    out[...] = found.astype(bf16)


def index(holders, slots, lengths, spread, live, gather, order):
    mine = lax.axis_index("dp") * MP + lax.axis_index("mp")

    def rows_of(array, count):
        row = iota((count, TOTAL), 0)
        rows = jnp.zeros((count, TOTAL), i32)
        for j in range(PMAX):
            rows = jnp.where(row % PMAX == j, array[j : j + 1], rows)
        return rows

    def held(count, group):
        lane = iota((count, TOTAL), 1)
        return (rows_of(holders[...], count) == mine) & (lane // SEQ == group)

    def total(mask, values):
        return jnp.sum(jnp.where(mask, values, 0), axis=1, keepdims=True)

    row = iota((HEAD, TOTAL), 0)
    lane = iota((HEAD, TOTAL), 1)
    mask = held(HEAD, row // (GROUPS * PMAX))
    slot = total(mask, rows_of(slots[...], HEAD))
    length = total(mask, lengths[...])
    count = jnp.clip(length - PAGE * (iota((HEAD, 1), 0) % PMAX), 0, PAGE)
    match = (slot == lane // 8) & ((row // PMAX) % GROUPS == lane % GROUPS)
    turned = jnp.where(match, 1.0, 0.0).T.astype(bf16)
    spread[...] = turned
    live[...] = dot(turned, jnp.broadcast_to(count.astype(f32), (HEAD, HEAD)).astype(bf16))

    row = iota((TOTAL, TOTAL), 0)
    mask = held(TOTAL, row // SEQ)
    slot = total(mask, rows_of(slots[...], TOTAL))
    row = iota((TOTAL, 1), 0)
    target = slot * 8 + (row // 8) % GROUPS + jnp.where(row % 8 < PMAX, 0, TOTAL)
    gather[...] = one_hot(target == iota((TOTAL, 2 * TOTAL), 1))

    first = lax.axis_index("dp") * SEQ
    lane = iota((8, TOTAL), 1)
    named = jnp.zeros((8, TOTAL), i32)
    table = jnp.concatenate([holders[...]] * 2, axis=0)
    for r in range(8):
        rolled = pltpu.roll(table, (TOTAL - first + r * SEQ) % TOTAL, 1)
        named = jnp.where(lane // SEQ == r, rolled[r % PMAX : r % PMAX + 1], named)
    lane = iota((TOTAL, TOTAL), 1)
    match = named[0:1] * 8 + lane // SEQ == iota((TOTAL, TOTAL), 0)
    order[...] = jnp.where(match, 1.0, 0.0).T.astype(bf16)


def route(ids, values, picks, scatter, weights):
    core = lax.axis_index("core")
    own_x = lax.axis_index("x")
    expert = (iota((8, TOTAL), 0) % NX) * NC + core
    member = jnp.where((ids[0:1] == expert) | (ids[1:2] == expert), 1.0, 0.0)
    row = iota((TOTAL, TOTAL), 0)
    lane = iota((TOTAL, TOTAL), 1)
    before = one_hot((row < lane) & (row // SEQ == lane // SEQ))
    rank = dot(member.astype(bf16), before)
    row = iota((ROWS, TOTAL), 0)
    lane = iota((ROWS, TOTAL), 1)
    place = (row % CAP).astype(f32)
    own = jnp.zeros((ROWS, TOTAL), f32)
    for k in range(NX):
        match = (member[k : k + 1] > 0.5) & (rank[k : k + 1] == place)
        match = jnp.where(match & (lane // SEQ == row // CAP), 1.0, 0.0)
        picks[k * ROWS : (k + 1) * ROWS] = match.astype(bf16)
        own = jnp.where(own_x == k, match, own)
    chosen = own_x * NC + core
    value = jnp.sum(jnp.where(ids[...] == chosen, values[...], 0.0), axis=0, keepdims=True)
    weight = jnp.sum(own * value, axis=1, keepdims=True)
    weights[...] = jnp.broadcast_to(weight, (ROWS, HEAD))
    row = iota((TOTAL, TOTAL), 0)
    half = jnp.where(row < ROWS, 1 - core, core)
    chip = (row % ROWS) // DP
    token = (row % DP) * SEQ + (chip // MP) * (NC * MP) + half * MP + chip % MP
    order = one_hot(token == iota((TOTAL, TOTAL), 1))
    scatter[...] = dot(order, own.astype(bf16), ((1,), (1,))).astype(bf16)


STEP = 8
STEPS = SLOTS // STEP
EARLY = 2


def prepare_kernel(
    after, holders, slots, lengths, ids, values, pages, *outs_and_sem
):
    del after
    spread, live, gather, order, picks, scatter, weights, held, sem = outs_and_sem
    copy = pltpu.make_async_copy(pages.at[0, pl.ds(0, EARLY * STEP)], held, sem)
    copy.start()
    index(holders, slots, lengths, spread, live, gather, order)
    route(ids, values, picks, scatter, weights)
    copy.wait()


def attend_kernel(queries, spread, live, gather, early, pages, out, parts, late, sems):
    copies = [
        pltpu.make_async_copy(
            pages.at[0, pl.ds((EARLY + k) * STEP, STEP)],
            late.at[pl.ds(k * STEP, STEP)],
            sems.at[k],
        )
        for k in range(STEPS - EARLY)
    ]
    for copy in copies:
        copy.start()
    for step in range(STEPS):
        rows = slice(step * STEP * 8, (step + 1) * STEP * 8)
        wanted = dot(spread[rows], queries[...])
        held = early if step < EARLY else late
        first_page = (step if step < EARLY else step - EARLY) * STEP
        if step >= EARLY:
            copies[step - EARLY].wait()
        scores = jnp.concatenate(
            [
                dot(
                    wanted[k * 8 : (k + 1) * 8].astype(bf16),
                    held[first_page + k, 0],
                    ((1,), (1,)),
                )
                for k in range(STEP)
            ],
            axis=0,
        )
        scores = scores * SCALE
        position = iota((STEP * 8, PAGE), 1).astype(f32)
        is_live = position < live[rows, 0:1]
        masked = jnp.where(is_live, scores, FLOOR)
        top = jnp.max(masked, axis=1, keepdims=True).astype(bf16).astype(f32)
        weights = jnp.where(is_live, jnp.exp(masked - top), 0.0)
        total = jnp.sum(weights, axis=1, keepdims=True)
        coarse = weights.astype(bf16).astype(f32)
        first = iota((STEP * 8, PAGE), 0) % 8 < GROUPS
        split = jnp.where(first, coarse, weights - coarse)
        found = []
        for k in range(STEP):
            both = dot(split[k * 8 : (k + 1) * 8].astype(bf16), held[first_page + k, 1])
            found.append(both + pltpu.roll(both, GROUPS, 0))
        parts[rows, :] = jnp.concatenate(found, axis=0)
        lane = iota((STEP * 8, HEAD), 1)
        high = total.astype(bf16).astype(f32)
        tops = jnp.where(lane < 64, top, jnp.where(lane < 96, high, total - high))
        parts[TOTAL + step * STEP * 8 : TOTAL + (step + 1) * STEP * 8, :] = tops
    out[...] = dot(gather[...], parts[...].astype(bf16)).astype(bf16)


def project_kernel(received, queries, fresh, order, weight, out):
    head = pl.multiple_of(lax.axis_index("mp") * HEAD, HEAD)
    sorted_parts = dot(order[...], received[...])
    pages = [sorted_parts[j * SEQ : (j + 1) * SEQ] for j in range(PMAX)]
    scalars = [sorted_parts[(PMAX + j) * SEQ : (PMAX + j + 1) * SEQ] for j in range(PMAX)]
    asked = queries[:, pl.ds(head, HEAD)].astype(f32)
    own = jnp.sum(asked * fresh[0].astype(f32), axis=1, keepdims=True) * SCALE
    highest = own
    for part in scalars:
        highest = jnp.maximum(highest, part[:, 0:1])
    factor = jnp.exp(own - highest)
    total = factor
    weighted = factor * fresh[1].astype(f32)
    for page, part in zip(pages, scalars):
        factor = jnp.exp(part[:, 0:1] - highest)
        total = total + (part[:, 64:65] + part[:, 96:97]) * factor
        weighted = weighted + page * factor
    attended = (weighted / total).astype(bf16)
    for k in range(CHIPS):
        out[k] = dot(attended, weight[:, k * COLS : (k + 1) * COLS]).astype(bf16)


def sum_kernel(received, mine, sent):
    summed = jnp.sum(received[...].astype(f32), axis=0)
    mine[...] = summed
    sent[...] = summed.astype(bf16)


def residual_kernel(mine, theirs, tokens, gain, out, plain):
    chip = lax.axis_index("x") * MP + lax.axis_index("mp")
    cols = pl.ds(pl.multiple_of(chip * COLS, COLS), COLS)
    total = mine[...] + theirs[...].astype(f32) + tokens[:, cols].astype(f32)
    gained = (total * gain[:, cols]).astype(bf16)
    out[...] = jnp.broadcast_to(gained[None], (DP, SEQ, COLS))
    lines = total.reshape(NX, NC * MP, COLS)
    turned = jnp.concatenate([lines[:, MP:], lines[:, :MP]], axis=1)
    plain[...] = jnp.where(lax.axis_index("core") == 0, lines, turned)


def pick_kernel(rows, picks, out):
    for k in range(NX):
        block = dot(picks[k * ROWS : (k + 1) * ROWS], rows[...]).astype(bf16)
        for m in range(MP):
            out[k * MP + m] = block


def hidden_kernel(rows, gain, gate, up, scatter, weights, weight, out, mine):
    part = jnp.concatenate([rows[k] for k in range(CHIPS)], axis=1)
    gate_sum = dot(part, gate[0])
    up_sum = dot(part, up[0])
    inverse = 1.0 / gain[...]
    squares = jnp.zeros((ROWS, COLS), f32)
    for k in range(CHIPS):
        plain = rows[k].astype(f32) * inverse[:, k * COLS : (k + 1) * COLS]
        squares = squares + plain * plain
    mean = jnp.sum(squares, axis=1, keepdims=True) * (1.0 / D)
    scale = lax.rsqrt(mean + 1e-05)
    gated = gate_sum * scale
    value = gated / (1.0 + jnp.exp(-gated)) * (up_sum * scale)
    value = (value * weights[:, 0:1]).astype(bf16)
    hidden = dot(scatter[...], value).astype(bf16)
    mine[...] = hidden[ROWS:]
    for k in range(CHIPS):
        cols = slice(k * COLS, (k + 1) * COLS)
        block = dot(hidden[:ROWS], weight[0, :, cols]).reshape(CHIPS, DP, COLS)
        out[:, k * DP : (k + 1) * DP, :] = block.astype(bf16)


def down_kernel(hidden, weight, out):
    for k in range(CHIPS):
        cols = slice(k * COLS, (k + 1) * COLS)
        block = dot(hidden[...], weight[0, :, cols]).reshape(CHIPS, DP, COLS)
        out[:, k * DP : (k + 1) * DP, :] = block.astype(bf16)


def join_kernel(mine, theirs, plain, out):
    chip = lax.axis_index("x") * MP + lax.axis_index("mp")
    at = iota((ROWS, COLS), 0) == chip * DP + lax.axis_index("dp")
    for k in range(CHIPS):
        line = plain[k // MP, k % MP : k % MP + 1, :]
        total = mine[k].astype(f32) + theirs[k].astype(f32)
        out[k] = (total + jnp.where(at, line, 0.0)).astype(bf16)


def chip_sum_kernel(received, out):
    for k in range(CHIPS):
        summed = jnp.sum(received[:, k * DP : (k + 1) * DP, :].astype(f32), axis=0)
        out[:, 2 * k : 2 * k + 2, :] = summed.reshape(DP, 2, HEAD).astype(bf16)


def final_kernel(received, out):
    summed = jnp.sum(received[...].astype(f32), axis=0)
    for k in range(D // HEAD):
        out[:, k * HEAD : (k + 1) * HEAD] = summed[k : k + 1].astype(bf16)


def call(kernel, out_shape, arrays, scratch=(), limit=8, hbm=(), name=None):
    vmem = pl.BlockSpec(memory_space=pltpu.VMEM)
    anywhere = pl.BlockSpec(memory_space=pl.ANY)
    return pl.pallas_call(
        kernel,
        out_shape=out_shape,
        in_specs=[anywhere if k in hbm else vmem for k in range(len(arrays))],
        out_specs=jax.tree.map(lambda _: vmem, out_shape),
        scratch_shapes=scratch,
        compiler_params=pltpu.CompilerParams(vmem_limit_bytes=limit * 2**20),
        name=name,
    )(*arrays)


def struct(shape, dtype=bf16):
    return jax.ShapeDtypeStruct(shape, dtype)


def in_hbm(array):
    return pltpu.with_memory_space_constraint(array, pltpu.HBM)


def exchange(array, axes):
    return lax.all_to_all(array, axes, 0, 0, tiled=True)


def swap(array):
    return lax.ppermute(array, "core", [(0, 1), (1, 0)])


def body(
    queries,
    fresh_entries,
    page_cache,
    lengths,
    page_holder,
    page_slot,
    tokens,
    norm_gain,
    out_weight,
    expert_ids,
    gate_values,
    gate_weight,
    up_weight,
    down_weight,
):
    gain = norm_gain.reshape(1, D)
    holders = page_holder.T

    lines = DP * GROUPS * PMAX
    selected = call(
        select_kernel,
        struct((lines, HEAD)),
        (in_hbm(queries), in_hbm(holders)),
        name="select",
    )
    asked = exchange(selected.reshape(DP, GROUPS * PMAX, HEAD), "dp").reshape(lines, HEAD)
    spread, live, gather, order, picks, scatter, weights, early = call(
        prepare_kernel,
        (
            struct((TOTAL, HEAD)),
            struct((TOTAL, HEAD), f32),
            struct((TOTAL, 2 * TOTAL)),
            struct((TOTAL, TOTAL)),
            struct((NX * ROWS, TOTAL)),
            struct((TOTAL, ROWS)),
            struct((ROWS, HEAD), f32),
            struct((EARLY * STEP, *page_cache.shape[2:])),
        ),
        (
            selected,
            in_hbm(holders),
            in_hbm(page_slot.T),
            in_hbm(lengths.reshape(1, TOTAL)),
            in_hbm(expert_ids.T),
            in_hbm(gate_values.T),
            in_hbm(page_cache),
        ),
        scratch=[pltpu.SemaphoreType.DMA(())],
        hbm=(0, 6),
        name="prepare",
    )
    parts = call(
        attend_kernel,
        struct((TOTAL, HEAD)),
        (asked, spread, live, gather, early, in_hbm(page_cache)),
        scratch=[
            pltpu.VMEM((2 * TOTAL, HEAD), f32),
            pltpu.VMEM(((STEPS - EARLY) * STEP, *page_cache.shape[2:]), bf16),
            pltpu.SemaphoreType.DMA((STEPS - EARLY,)),
        ],
        hbm=(5,),
        name="attend",
    )
    parts = exchange(parts.reshape(HOLDERS, 8, HEAD), ("dp", "mp")).reshape(TOTAL, HEAD)

    projected = call(
        project_kernel,
        struct((CHIPS, SEQ, COLS)),
        (parts, queries, fresh_entries, order, out_weight),
        name="project",
    )
    projected = exchange(projected, ("x", "mp"))
    mine, sent = call(
        sum_kernel,
        (struct((SEQ, COLS), f32), struct((SEQ, COLS))),
        (projected,),
        name="sum_heads",
    )

    gained, plain = call(
        residual_kernel,
        (struct((DP, SEQ, COLS)), struct((NX, NC * MP, COLS), f32)),
        (mine, swap(sent), tokens, gain),
        name="residual",
    )
    gained = exchange(gained, "dp").reshape(TOTAL, COLS)
    picked = call(pick_kernel, struct((CHIPS, ROWS, COLS)), (gained, picks), name="pick")
    rows = exchange(picked, ("x", "mp"))
    other_out, own_hidden = call(
        hidden_kernel,
        (struct((CHIPS, ROWS, COLS)), struct((ROWS, FF))),
        (rows, gain, gate_weight, up_weight, scatter, weights, down_weight),
        name="hidden",
    )
    passed = swap(other_out)
    own_out = call(
        down_kernel, struct((CHIPS, ROWS, COLS)), (own_hidden, down_weight), name="down"
    )

    summed = call(
        join_kernel, struct((CHIPS, ROWS, COLS)), (own_out, passed, plain), name="join"
    )
    summed = exchange(summed, ("x", "mp"))
    lines = call(chip_sum_kernel, struct((DP, D // HEAD, HEAD)), (summed,), name="chip_sum")
    lines = exchange(lines, "dp")
    return call(final_kernel, struct((1, D)), (lines,), name="final")


def solution(mesh):
    fine = Mesh(mesh.devices.reshape(DP, NX, NC, MP), ("dp", "x", "core", "mp"))
    expert = ("x", "core")
    return jax.shard_map(
        body,
        mesh=fine,
        in_specs=(
            P("dp", expert),
            P(None, "dp", expert),
            P(expert, ("dp", "mp"), None, None, None),
            P(),
            P(),
            P(),
            P("dp", None),
            P(),
            P((*expert, "mp"), None),
            P(),
            P(),
            P(expert, None, ("dp", "mp")),
            P(expert, None, ("dp", "mp")),
            P(expert, ("dp", "mp"), None),
        ),
        out_specs=P(("dp", *expert, "mp"), None),
        check_vma=False,
    )
```

```python
import jax
import jax.numpy as jnp
from jax import lax
from jax.experimental import pallas as pl
from jax.experimental.pallas import tpu as pltpu
from jax.sharding import Mesh, PartitionSpec as P

bf16 = jnp.bfloat16
f32 = jnp.float32
i32 = jnp.int32

DP, NX, NC, MP = 8, 4, 2, 4
EXPERTS = NX * NC
HOLDERS = DP * MP
PMAX = 4
SEQ = 32
TOTAL = DP * SEQ
SLOTS = 32
PAGE = 256
HEAD = 128
GROUPS = 4
D = 4096
FF = 256
CAP = 16
CHIPS = NX * MP
COLS = D // CHIPS
HALF = SEQ // NC
ROWS = DP * HALF
FLOOR = -1e30
SCALE = HEAD ** (-0.5)


def iota(shape, dim):
    return lax.broadcasted_iota(i32, shape, dim)


def dot(a, b, dims=((1,), (0,))):
    return lax.dot_general(a, b, (dims, ((), ())), preferred_element_type=f32)


def one_hot(mask):
    return jnp.where(mask, 1.0, 0.0).astype(bf16)


def select_kernel(queries, holders, out):
    first = lax.axis_index("dp") * SEQ
    table = pltpu.roll(holders[...], (TOTAL - first) % TOTAL, 1)[:, :SEQ]
    row = iota((HEAD, SEQ), 0)
    named = jnp.zeros((HEAD, SEQ), i32)
    for j in range(PMAX):
        named = jnp.where(row % PMAX == j, table[j : j + 1], named)
    wanted = (row // (GROUPS * PMAX)) * MP + lax.axis_index("mp")
    found = jnp.zeros((HEAD, HEAD), f32)
    for k in range(GROUPS):
        pick = one_hot((named == wanted) & ((row // PMAX) % GROUPS == k))
        found = found + dot(pick, queries[:, k * HEAD : (k + 1) * HEAD])
    out[...] = found.astype(bf16)


def index(holders, slots, lengths, spread, live, gather, order):
    mine = lax.axis_index("dp") * MP + lax.axis_index("mp")

    def rows_of(array, count):
        row = iota((count, TOTAL), 0)
        rows = jnp.zeros((count, TOTAL), i32)
        for j in range(PMAX):
            rows = jnp.where(row % PMAX == j, array[j : j + 1], rows)
        return rows

    def held(count, group):
        lane = iota((count, TOTAL), 1)
        return (rows_of(holders[...], count) == mine) & (lane // SEQ == group)

    def total(mask, values):
        return jnp.sum(jnp.where(mask, values, 0), axis=1, keepdims=True)

    row = iota((HEAD, TOTAL), 0)
    lane = iota((HEAD, TOTAL), 1)
    mask = held(HEAD, row // (GROUPS * PMAX))
    slot = total(mask, rows_of(slots[...], HEAD))
    length = total(mask, lengths[...])
    count = jnp.clip(length - PAGE * (iota((HEAD, 1), 0) % PMAX), 0, PAGE)
    match = (slot == lane // 8) & ((row // PMAX) % GROUPS == lane % GROUPS)
    turned = jnp.where(match, 1.0, 0.0).T.astype(bf16)
    spread[...] = turned
    live[...] = dot(turned, jnp.broadcast_to(count.astype(f32), (HEAD, HEAD)).astype(bf16))

    row = iota((TOTAL, TOTAL), 0)
    mask = held(TOTAL, row // SEQ)
    slot = total(mask, rows_of(slots[...], TOTAL))
    row = iota((TOTAL, 1), 0)
    target = slot * 8 + (row // 8) % GROUPS + jnp.where(row % 8 < PMAX, 0, TOTAL)
    gather[...] = one_hot(target == iota((TOTAL, 2 * TOTAL), 1))

    first = lax.axis_index("dp") * SEQ
    lane = iota((8, TOTAL), 1)
    named = jnp.zeros((8, TOTAL), i32)
    table = jnp.concatenate([holders[...]] * 2, axis=0)
    for r in range(8):
        rolled = pltpu.roll(table, (TOTAL - first + r * SEQ) % TOTAL, 1)
        named = jnp.where(lane // SEQ == r, rolled[r % PMAX : r % PMAX + 1], named)
    lane = iota((TOTAL, TOTAL), 1)
    match = named[0:1] * 8 + lane // SEQ == iota((TOTAL, TOTAL), 0)
    order[...] = jnp.where(match, 1.0, 0.0).T.astype(bf16)


def route(ids, values, picks, scatter, weights):
    core = lax.axis_index("core")
    own_x = lax.axis_index("x")
    expert = (iota((8, TOTAL), 0) % NX) * NC + core
    member = jnp.where((ids[0:1] == expert) | (ids[1:2] == expert), 1.0, 0.0)
    row = iota((TOTAL, TOTAL), 0)
    lane = iota((TOTAL, TOTAL), 1)
    before = one_hot((row < lane) & (row // SEQ == lane // SEQ))
    rank = dot(member.astype(bf16), before)
    row = iota((ROWS, TOTAL), 0)
    lane = iota((ROWS, TOTAL), 1)
    place = (row % CAP).astype(f32)
    own = jnp.zeros((ROWS, TOTAL), f32)
    for k in range(NX):
        match = (member[k : k + 1] > 0.5) & (rank[k : k + 1] == place)
        match = jnp.where(match & (lane // SEQ == row // CAP), 1.0, 0.0)
        picks[k * ROWS : (k + 1) * ROWS] = match.astype(bf16)
        own = jnp.where(own_x == k, match, own)
    chosen = own_x * NC + core
    value = jnp.sum(jnp.where(ids[...] == chosen, values[...], 0.0), axis=0, keepdims=True)
    weight = jnp.sum(own * value, axis=1, keepdims=True)
    weights[...] = jnp.broadcast_to(weight, (ROWS, HEAD))
    row = iota((TOTAL, TOTAL), 0)
    half = jnp.where(row < ROWS, 1 - core, core)
    chip = (row % ROWS) // DP
    token = (row % DP) * SEQ + (chip // MP) * (NC * MP) + half * MP + chip % MP
    order = one_hot(token == iota((TOTAL, TOTAL), 1))
    scatter[...] = dot(order, own.astype(bf16), ((1,), (1,))).astype(bf16)


STEP = 8
STEPS = SLOTS // STEP
EARLY = 2


def prepare_kernel(
    after, holders, slots, lengths, ids, values, pages, *outs_and_sem
):
    del after
    spread, live, gather, order, picks, scatter, weights, held, sem = outs_and_sem
    copy = pltpu.make_async_copy(pages.at[0, pl.ds(0, EARLY * STEP)], held, sem)
    copy.start()
    index(holders, slots, lengths, spread, live, gather, order)
    route(ids, values, picks, scatter, weights)
    copy.wait()


def attend_kernel(queries, spread, live, gather, early, pages, out, parts, late, sems):
    copies = [
        pltpu.make_async_copy(
            pages.at[0, pl.ds((EARLY + k) * STEP, STEP)],
            late.at[pl.ds(k * STEP, STEP)],
            sems.at[k],
        )
        for k in range(STEPS - EARLY)
    ]
    for copy in copies:
        copy.start()
    for step in range(STEPS):
        rows = slice(step * STEP * 8, (step + 1) * STEP * 8)
        wanted = dot(spread[rows], queries[...])
        held = early if step < EARLY else late
        first_page = (step if step < EARLY else step - EARLY) * STEP
        if step >= EARLY:
            copies[step - EARLY].wait()
        scores = jnp.concatenate(
            [
                dot(
                    wanted[k * 8 : (k + 1) * 8].astype(bf16),
                    held[first_page + k, 0],
                    ((1,), (1,)),
                )
                for k in range(STEP)
            ],
            axis=0,
        )
        scores = scores * SCALE
        position = iota((STEP * 8, PAGE), 1).astype(f32)
        is_live = position < live[rows, 0:1]
        masked = jnp.where(is_live, scores, FLOOR)
        top = jnp.max(masked, axis=1, keepdims=True).astype(bf16).astype(f32)
        weights = jnp.where(is_live, jnp.exp(masked - top), 0.0)
        total = jnp.sum(weights, axis=1, keepdims=True)
        coarse = weights.astype(bf16).astype(f32)
        first = iota((STEP * 8, PAGE), 0) % 8 < GROUPS
        split = jnp.where(first, coarse, weights - coarse)
        found = []
        for k in range(STEP):
            both = dot(split[k * 8 : (k + 1) * 8].astype(bf16), held[first_page + k, 1])
            found.append(both + pltpu.roll(both, GROUPS, 0))
        parts[rows, :] = jnp.concatenate(found, axis=0)
        lane = iota((STEP * 8, HEAD), 1)
        high = total.astype(bf16).astype(f32)
        tops = jnp.where(lane < 64, top, jnp.where(lane < 96, high, total - high))
        parts[TOTAL + step * STEP * 8 : TOTAL + (step + 1) * STEP * 8, :] = tops
    out[...] = dot(gather[...], parts[...].astype(bf16)).astype(bf16)


def project_kernel(received, queries, fresh, order, weight, out):
    head = pl.multiple_of(lax.axis_index("mp") * HEAD, HEAD)
    sorted_parts = dot(order[...], received[...])
    pages = [sorted_parts[j * SEQ : (j + 1) * SEQ] for j in range(PMAX)]
    scalars = [sorted_parts[(PMAX + j) * SEQ : (PMAX + j + 1) * SEQ] for j in range(PMAX)]
    asked = queries[:, pl.ds(head, HEAD)].astype(f32)
    own = jnp.sum(asked * fresh[0].astype(f32), axis=1, keepdims=True) * SCALE
    highest = own
    for part in scalars:
        highest = jnp.maximum(highest, part[:, 0:1])
    factor = jnp.exp(own - highest)
    total = factor
    weighted = factor * fresh[1].astype(f32)
    for page, part in zip(pages, scalars):
        factor = jnp.exp(part[:, 0:1] - highest)
        total = total + (part[:, 64:65] + part[:, 96:97]) * factor
        weighted = weighted + page * factor
    attended = (weighted / total).astype(bf16)
    for k in range(CHIPS):
        out[k] = dot(attended, weight[:, k * COLS : (k + 1) * COLS]).astype(bf16)


def core_sum_kernel(mine, theirs, out):
    out[...] = (mine[...].astype(f32) + theirs[...].astype(f32)).astype(bf16)


def residual_kernel(received, tokens, gain, out, plain):
    chip = lax.axis_index("x") * MP + lax.axis_index("mp")
    cols = pl.ds(pl.multiple_of(chip * COLS, COLS), COLS)
    total = jnp.sum(received[...].astype(f32), axis=0) + tokens[:, cols].astype(f32)
    gained = (total * gain[:, cols]).astype(bf16)
    out[...] = jnp.broadcast_to(gained[None], (DP, SEQ, COLS))
    lines = total.reshape(NX, NC * MP, COLS)
    turned = jnp.concatenate([lines[:, MP:], lines[:, :MP]], axis=1)
    plain[...] = jnp.where(lax.axis_index("core") == 0, lines, turned)


def pick_kernel(rows, picks, out):
    for k in range(NX):
        block = dot(picks[k * ROWS : (k + 1) * ROWS], rows[...]).astype(bf16)
        for m in range(MP):
            out[k * MP + m] = block


def hidden_kernel(rows, gain, gate, up, scatter, weights, weight, out, mine):
    part = jnp.concatenate([rows[k] for k in range(CHIPS)], axis=1)
    gate_sum = dot(part, gate[0])
    up_sum = dot(part, up[0])
    inverse = 1.0 / gain[...]
    squares = jnp.zeros((ROWS, COLS), f32)
    for k in range(CHIPS):
        plain = rows[k].astype(f32) * inverse[:, k * COLS : (k + 1) * COLS]
        squares = squares + plain * plain
    mean = jnp.sum(squares, axis=1, keepdims=True) * (1.0 / D)
    scale = lax.rsqrt(mean + 1e-05)
    gated = gate_sum * scale
    value = gated / (1.0 + jnp.exp(-gated)) * (up_sum * scale)
    value = (value * weights[:, 0:1]).astype(bf16)
    hidden = dot(scatter[...], value).astype(bf16)
    mine[...] = hidden[ROWS:]
    for k in range(CHIPS):
        cols = slice(k * COLS, (k + 1) * COLS)
        block = dot(hidden[:ROWS], weight[0, :, cols]).reshape(CHIPS, DP, COLS)
        out[:, k * DP : (k + 1) * DP, :] = block.astype(bf16)


def down_kernel(hidden, weight, out):
    for k in range(CHIPS):
        cols = slice(k * COLS, (k + 1) * COLS)
        block = dot(hidden[...], weight[0, :, cols]).reshape(CHIPS, DP, COLS)
        out[:, k * DP : (k + 1) * DP, :] = block.astype(bf16)


def join_kernel(mine, theirs, plain, out):
    chip = lax.axis_index("x") * MP + lax.axis_index("mp")
    at = iota((ROWS, COLS), 0) == chip * DP + lax.axis_index("dp")
    for k in range(CHIPS):
        line = plain[k // MP, k % MP : k % MP + 1, :]
        total = mine[k].astype(f32) + theirs[k].astype(f32)
        out[k] = (total + jnp.where(at, line, 0.0)).astype(bf16)


def chip_sum_kernel(received, out):
    for k in range(CHIPS):
        summed = jnp.sum(received[:, k * DP : (k + 1) * DP, :].astype(f32), axis=0)
        out[:, 2 * k : 2 * k + 2, :] = summed.reshape(DP, 2, HEAD).astype(bf16)


def final_kernel(received, out):
    summed = jnp.sum(received[...].astype(f32), axis=0)
    for k in range(D // HEAD):
        out[:, k * HEAD : (k + 1) * HEAD] = summed[k : k + 1].astype(bf16)


def call(kernel, out_shape, arrays, scratch=(), limit=8, hbm=(), name=None):
    vmem = pl.BlockSpec(memory_space=pltpu.VMEM)
    anywhere = pl.BlockSpec(memory_space=pl.ANY)
    return pl.pallas_call(
        kernel,
        out_shape=out_shape,
        in_specs=[anywhere if k in hbm else vmem for k in range(len(arrays))],
        out_specs=jax.tree.map(lambda _: vmem, out_shape),
        scratch_shapes=scratch,
        compiler_params=pltpu.CompilerParams(vmem_limit_bytes=limit * 2**20),
        name=name,
    )(*arrays)


def struct(shape, dtype=bf16):
    return jax.ShapeDtypeStruct(shape, dtype)


def in_hbm(array):
    return pltpu.with_memory_space_constraint(array, pltpu.HBM)


def exchange(array, axes):
    return lax.all_to_all(array, axes, 0, 0, tiled=True)


def swap(array):
    return lax.ppermute(array, "core", [(0, 1), (1, 0)])


def body(
    queries,
    fresh_entries,
    page_cache,
    lengths,
    page_holder,
    page_slot,
    tokens,
    norm_gain,
    out_weight,
    expert_ids,
    gate_values,
    gate_weight,
    up_weight,
    down_weight,
):
    gain = norm_gain.reshape(1, D)
    holders = page_holder.T

    lines = DP * GROUPS * PMAX
    selected = call(
        select_kernel,
        struct((lines, HEAD)),
        (in_hbm(queries), in_hbm(holders)),
        name="select",
    )
    asked = exchange(selected.reshape(DP, GROUPS * PMAX, HEAD), "dp").reshape(lines, HEAD)
    spread, live, gather, order, picks, scatter, weights, early = call(
        prepare_kernel,
        (
            struct((TOTAL, HEAD)),
            struct((TOTAL, HEAD), f32),
            struct((TOTAL, 2 * TOTAL)),
            struct((TOTAL, TOTAL)),
            struct((NX * ROWS, TOTAL)),
            struct((TOTAL, ROWS)),
            struct((ROWS, HEAD), f32),
            struct((EARLY * STEP, *page_cache.shape[2:])),
        ),
        (
            selected,
            in_hbm(holders),
            in_hbm(page_slot.T),
            in_hbm(lengths.reshape(1, TOTAL)),
            in_hbm(expert_ids.T),
            in_hbm(gate_values.T),
            in_hbm(page_cache),
        ),
        scratch=[pltpu.SemaphoreType.DMA(())],
        hbm=(0, 6),
        name="prepare",
    )
    parts = call(
        attend_kernel,
        struct((TOTAL, HEAD)),
        (asked, spread, live, gather, early, in_hbm(page_cache)),
        scratch=[
            pltpu.VMEM((2 * TOTAL, HEAD), f32),
            pltpu.VMEM(((STEPS - EARLY) * STEP, *page_cache.shape[2:]), bf16),
            pltpu.SemaphoreType.DMA((STEPS - EARLY,)),
        ],
        hbm=(5,),
        name="attend",
    )
    parts = exchange(parts.reshape(HOLDERS, 8, HEAD), ("dp", "mp")).reshape(TOTAL, HEAD)

    projected = call(
        project_kernel,
        struct((CHIPS, SEQ, COLS)),
        (parts, queries, fresh_entries, order, out_weight),
        name="project",
    )
    projected = call(
        core_sum_kernel,
        struct((CHIPS, SEQ, COLS)),
        (projected, swap(projected)),
        name="core_sum",
    )
    projected = exchange(projected, ("x", "mp"))

    gained, plain = call(
        residual_kernel,
        (struct((DP, SEQ, COLS)), struct((NX, NC * MP, COLS), f32)),
        (projected, tokens, gain),
        name="residual",
    )
    gained = exchange(gained, "dp").reshape(TOTAL, COLS)
    picked = call(pick_kernel, struct((CHIPS, ROWS, COLS)), (gained, picks), name="pick")
    rows = exchange(picked, ("x", "mp"))
    other_out, own_hidden = call(
        hidden_kernel,
        (struct((CHIPS, ROWS, COLS)), struct((ROWS, FF))),
        (rows, gain, gate_weight, up_weight, scatter, weights, down_weight),
        name="hidden",
    )
    passed = swap(other_out)
    own_out = call(
        down_kernel, struct((CHIPS, ROWS, COLS)), (own_hidden, down_weight), name="down"
    )

    summed = call(
        join_kernel, struct((CHIPS, ROWS, COLS)), (own_out, passed, plain), name="join"
    )
    summed = exchange(summed, ("x", "mp"))
    lines = call(chip_sum_kernel, struct((DP, D // HEAD, HEAD)), (summed,), name="chip_sum")
    lines = exchange(lines, "dp")
    return call(final_kernel, struct((1, D)), (lines,), name="final")


def solution(mesh):
    fine = Mesh(mesh.devices.reshape(DP, NX, NC, MP), ("dp", "x", "core", "mp"))
    expert = ("x", "core")
    return jax.shard_map(
        body,
        mesh=fine,
        in_specs=(
            P("dp", expert),
            P(None, "dp", expert),
            P(expert, ("dp", "mp"), None, None, None),
            P(),
            P(),
            P(),
            P("dp", None),
            P(),
            P((*expert, "mp"), None),
            P(),
            P(),
            P(expert, None, ("dp", "mp")),
            P(expert, None, ("dp", "mp")),
            P(expert, ("dp", "mp"), None),
        ),
        out_specs=P(("dp", *expert, "mp"), None),
        check_vma=False,
    )
```

```python
import jax
import jax.numpy as jnp
from jax import lax
from jax.experimental import pallas as pl
from jax.experimental.pallas import tpu as pltpu
from jax.sharding import Mesh, PartitionSpec as P


bf16 = jnp.bfloat16
f32 = jnp.float32
i32 = jnp.int32

DP, NX, NC, MP = 8, 4, 2, 4
HOLDERS = DP * MP
PMAX = 4
SEQ = 32
TOTAL = DP * SEQ
SLOTS = 32
PAGE = 256
HEAD = 128
GROUPS = 4
D = 4096
FF = 256
CAP = 16
CHIPS = NX * MP
COLS = D // CHIPS
HALF = SEQ // NC
ROWS = DP * HALF
FLOOR = -1e30
SCALE = HEAD ** (-0.5)


def iota(shape, dim):
    return lax.broadcasted_iota(i32, shape, dim)


def dot(a, b, dims=((1,), (0,))):
    return lax.dot_general(a, b, (dims, ((), ())), preferred_element_type=f32)


def one_hot(mask):
    return jnp.where(mask, 1.0, 0.0).astype(bf16)


def select_kernel(queries, holders, out):
    first = lax.axis_index("dp") * SEQ
    table = pltpu.roll(holders[...], (TOTAL - first) % TOTAL, 1)[:, :SEQ]
    row = iota((HEAD, SEQ), 0)
    named = jnp.zeros((HEAD, SEQ), i32)
    for j in range(PMAX):
        named = jnp.where(row % PMAX == j, table[j : j + 1], named)
    wanted = (row // (GROUPS * PMAX)) * MP + lax.axis_index("mp")
    found = jnp.zeros((HEAD, HEAD), f32)
    for k in range(GROUPS):
        pick = one_hot((named == wanted) & ((row // PMAX) % GROUPS == k))
        found = found + dot(pick, queries[:, k * HEAD : (k + 1) * HEAD])
    out[...] = found.astype(bf16)


def index(holders, slots, lengths, spread, live, gather, order):
    mine = lax.axis_index("dp") * MP + lax.axis_index("mp")

    def rows_of(array, count):
        row = iota((count, TOTAL), 0)
        rows = jnp.zeros((count, TOTAL), i32)
        for j in range(PMAX):
            rows = jnp.where(row % PMAX == j, array[j : j + 1], rows)
        return rows

    def held(count, group):
        lane = iota((count, TOTAL), 1)
        return (rows_of(holders[...], count) == mine) & (lane // SEQ == group)

    def total(mask, values):
        return jnp.sum(jnp.where(mask, values, 0), axis=1, keepdims=True)

    row = iota((HEAD, TOTAL), 0)
    lane = iota((HEAD, TOTAL), 1)
    mask = held(HEAD, row // (GROUPS * PMAX))
    slot = total(mask, rows_of(slots[...], HEAD))
    length = total(mask, lengths[...])
    count = jnp.clip(length - PAGE * (iota((HEAD, 1), 0) % PMAX), 0, PAGE)
    match = (slot == lane // 8) & ((row // PMAX) % GROUPS == lane % GROUPS)
    turned = jnp.where(match, 1.0, 0.0).T.astype(bf16)
    spread[...] = turned
    live[...] = dot(turned, jnp.broadcast_to(count.astype(f32), (HEAD, HEAD)).astype(bf16))

    row = iota((TOTAL, TOTAL), 0)
    mask = held(TOTAL, row // SEQ)
    slot = total(mask, rows_of(slots[...], TOTAL))
    row = iota((TOTAL, 1), 0)
    target = slot * 8 + (row // 8) % GROUPS + jnp.where(row % 8 < PMAX, 0, TOTAL)
    gather[...] = one_hot(target == iota((TOTAL, 2 * TOTAL), 1))

    first = lax.axis_index("dp") * SEQ
    lane = iota((8, TOTAL), 1)
    named = jnp.zeros((8, TOTAL), i32)
    table = jnp.concatenate([holders[...]] * 2, axis=0)
    for r in range(8):
        rolled = pltpu.roll(table, (TOTAL - first + r * SEQ) % TOTAL, 1)
        named = jnp.where(lane // SEQ == r, rolled[r % PMAX : r % PMAX + 1], named)
    lane = iota((TOTAL, TOTAL), 1)
    match = named[0:1] * 8 + lane // SEQ == iota((TOTAL, TOTAL), 0)
    order[...] = jnp.where(match, 1.0, 0.0).T.astype(bf16)


def route(ids, values, picks, scatter, weights):
    core = lax.axis_index("core")
    own_x = lax.axis_index("x")
    expert = (iota((8, TOTAL), 0) % NX) * NC + core
    member = jnp.where((ids[0:1] == expert) | (ids[1:2] == expert), 1.0, 0.0)
    row = iota((TOTAL, TOTAL), 0)
    lane = iota((TOTAL, TOTAL), 1)
    before = one_hot((row < lane) & (row // SEQ == lane // SEQ))
    rank = dot(member.astype(bf16), before)
    row = iota((ROWS, TOTAL), 0)
    lane = iota((ROWS, TOTAL), 1)
    place = (row % CAP).astype(f32)
    own = jnp.zeros((ROWS, TOTAL), f32)
    for k in range(NX):
        match = (member[k : k + 1] > 0.5) & (rank[k : k + 1] == place)
        match = jnp.where(match & (lane // SEQ == row // CAP), 1.0, 0.0)
        picks[k * ROWS : (k + 1) * ROWS] = match.astype(bf16)
        own = jnp.where(own_x == k, match, own)
    chosen = own_x * NC + core
    value = jnp.sum(jnp.where(ids[...] == chosen, values[...], 0.0), axis=0, keepdims=True)
    weight = jnp.sum(own * value, axis=1, keepdims=True)
    weights[...] = jnp.broadcast_to(weight, (ROWS, HEAD))
    row = iota((TOTAL, TOTAL), 0)
    half = jnp.where(row < ROWS, 1 - core, core)
    chip = (row % ROWS) // DP
    token = (row % DP) * SEQ + (chip // MP) * (NC * MP) + half * MP + chip % MP
    order = one_hot(token == iota((TOTAL, TOTAL), 1))
    scatter[...] = dot(order, own.astype(bf16), ((1,), (1,))).astype(bf16)


STEP = 8
STEPS = SLOTS // STEP
EARLY = 2


def prepare_kernel(
    after, holders, slots, lengths, ids, values, pages, *outs_and_sem
):
    del after
    spread, live, gather, order, picks, scatter, weights, held, sem = outs_and_sem
    copy = pltpu.make_async_copy(pages.at[0, pl.ds(0, EARLY * STEP)], held, sem)
    copy.start()
    index(holders, slots, lengths, spread, live, gather, order)
    route(ids, values, picks, scatter, weights)
    copy.wait()


def attend_kernel(queries, spread, live, gather, early, pages, out, parts, late, sems):
    copies = [
        pltpu.make_async_copy(
            pages.at[0, pl.ds((EARLY + k) * STEP, STEP)],
            late.at[pl.ds(k * STEP, STEP)],
            sems.at[k],
        )
        for k in range(STEPS - EARLY)
    ]
    for copy in copies:
        copy.start()
    for step in range(STEPS):
        rows = slice(step * STEP * 8, (step + 1) * STEP * 8)
        wanted = dot(spread[rows], queries[...])
        held = early if step < EARLY else late
        first_page = (step if step < EARLY else step - EARLY) * STEP
        if step >= EARLY:
            copies[step - EARLY].wait()
        scores = jnp.concatenate(
            [
                dot(
                    wanted[k * 8 : (k + 1) * 8].astype(bf16),
                    held[first_page + k, 0],
                    ((1,), (1,)),
                )
                for k in range(STEP)
            ],
            axis=0,
        )
        scores = scores * SCALE
        position = iota((STEP * 8, PAGE), 1).astype(f32)
        is_live = position < live[rows, 0:1]
        masked = jnp.where(is_live, scores, FLOOR)
        top = jnp.max(masked, axis=1, keepdims=True).astype(bf16).astype(f32)
        weights = jnp.where(is_live, jnp.exp(masked - top), 0.0)
        total = jnp.sum(weights, axis=1, keepdims=True)
        coarse = weights.astype(bf16).astype(f32)
        first = iota((STEP * 8, PAGE), 0) % 8 < GROUPS
        split = jnp.where(first, coarse, weights - coarse)
        found = []
        for k in range(STEP):
            both = dot(split[k * 8 : (k + 1) * 8].astype(bf16), held[first_page + k, 1])
            found.append(both + pltpu.roll(both, GROUPS, 0))
        parts[rows, :] = jnp.concatenate(found, axis=0)
        lane = iota((STEP * 8, HEAD), 1)
        high = total.astype(bf16).astype(f32)
        tops = jnp.where(lane < 64, top, jnp.where(lane < 96, high, total - high))
        parts[TOTAL + step * STEP * 8 : TOTAL + (step + 1) * STEP * 8, :] = tops
    out[...] = dot(gather[...], parts[...].astype(bf16)).astype(bf16)


def project_kernel(received, queries, fresh, order, weight, out, rows):
    head = pl.multiple_of(lax.axis_index("mp") * HEAD, HEAD)
    sorted_parts = dot(order[...], received[...])
    pages = [sorted_parts[j * SEQ : (j + 1) * SEQ] for j in range(PMAX)]
    scalars = [sorted_parts[(PMAX + j) * SEQ : (PMAX + j + 1) * SEQ] for j in range(PMAX)]
    asked = queries[:, pl.ds(head, HEAD)].astype(f32)
    own = jnp.sum(asked * fresh[0].astype(f32), axis=1, keepdims=True) * SCALE
    highest = own
    for part in scalars:
        highest = jnp.maximum(highest, part[:, 0:1])
    factor = jnp.exp(own - highest)
    total = factor
    weighted = factor * fresh[1].astype(f32)
    for page, part in zip(pages, scalars):
        factor = jnp.exp(part[:, 0:1] - highest)
        total = total + (part[:, 64:65] + part[:, 96:97]) * factor
        weighted = weighted + page * factor
    attended = (weighted / total).astype(bf16)
    rows[...] = attended
    for k in range(CHIPS // 2):
        out[k] = dot(attended, weight[:, k * COLS : (k + 1) * COLS]).astype(bf16)


def project_late_kernel(rows, weight, out):
    for k in range(CHIPS // 2):
        first = (CHIPS // 2 + k) * COLS
        out[k] = dot(rows[...], weight[:, first : first + COLS]).astype(bf16)


def core_sum_kernel(mine_a, mine_b, theirs_a, theirs_b, out):
    for first, mine, theirs in ((0, mine_a, theirs_a), (CHIPS // 2, mine_b, theirs_b)):
        total = mine[...].astype(f32) + theirs[...].astype(f32)
        out[first : first + CHIPS // 2] = total.astype(bf16)


def residual_kernel(received, tokens, gain, out, plain):
    chip = lax.axis_index("x") * MP + lax.axis_index("mp")
    cols = pl.ds(pl.multiple_of(chip * COLS, COLS), COLS)
    total = jnp.sum(received[...].astype(f32), axis=0) + tokens[:, cols].astype(f32)
    gained = (total * gain[:, cols]).astype(bf16)
    out[...] = jnp.broadcast_to(gained[None], (DP, SEQ, COLS))
    lines = total.reshape(NX, NC * MP, COLS)
    turned = jnp.concatenate([lines[:, MP:], lines[:, :MP]], axis=1)
    plain[...] = jnp.where(lax.axis_index("core") == 0, lines, turned)


def pick_kernel(rows, picks, out):
    for k in range(NX):
        block = dot(picks[k * ROWS : (k + 1) * ROWS], rows[...]).astype(bf16)
        for m in range(MP):
            out[k * MP + m] = block


def hidden_kernel(rows, gain, gate, up, scatter, weights, weight, out, mine):
    part = jnp.concatenate([rows[k] for k in range(CHIPS)], axis=1)
    gate_sum = dot(part, gate[0])
    up_sum = dot(part, up[0])
    inverse = 1.0 / gain[...]
    squares = jnp.zeros((ROWS, COLS), f32)
    for k in range(CHIPS):
        plain = rows[k].astype(f32) * inverse[:, k * COLS : (k + 1) * COLS]
        squares = squares + plain * plain
    mean = jnp.sum(squares, axis=1, keepdims=True) * (1.0 / D)
    scale = lax.rsqrt(mean + 1e-05)
    gated = gate_sum * scale
    value = gated / (1.0 + jnp.exp(-gated)) * (up_sum * scale)
    value = (value * weights[:, 0:1]).astype(bf16)
    hidden = dot(scatter[...], value).astype(bf16)
    mine[...] = hidden[ROWS:]
    for k in range(CHIPS):
        cols = slice(k * COLS, (k + 1) * COLS)
        block = dot(hidden[:ROWS], weight[0, :, cols]).reshape(CHIPS, DP, COLS)
        out[:, k * DP : (k + 1) * DP, :] = block.astype(bf16)


def down_kernel(hidden, weight, out):
    for k in range(CHIPS):
        cols = slice(k * COLS, (k + 1) * COLS)
        block = dot(hidden[...], weight[0, :, cols]).reshape(CHIPS, DP, COLS)
        out[:, k * DP : (k + 1) * DP, :] = block.astype(bf16)


def join_kernel(mine, theirs, plain, out):
    chip = lax.axis_index("x") * MP + lax.axis_index("mp")
    at = iota((ROWS, COLS), 0) == chip * DP + lax.axis_index("dp")
    for k in range(CHIPS):
        line = plain[k // MP, k % MP : k % MP + 1, :]
        total = mine[k].astype(f32) + theirs[k].astype(f32)
        out[k] = (total + jnp.where(at, line, 0.0)).astype(bf16)


def chip_sum_kernel(received, out):
    for k in range(CHIPS):
        summed = jnp.sum(received[:, k * DP : (k + 1) * DP, :].astype(f32), axis=0)
        out[:, 2 * k : 2 * k + 2, :] = summed.reshape(DP, 2, HEAD).astype(bf16)


def final_kernel(received, out):
    summed = jnp.sum(received[...].astype(f32), axis=0)
    for k in range(D // HEAD):
        out[:, k * HEAD : (k + 1) * HEAD] = summed[k : k + 1].astype(bf16)


def call(kernel, out_shape, arrays, scratch=(), limit=8, hbm=()):
    vmem = pl.BlockSpec(memory_space=pltpu.VMEM)
    anywhere = pl.BlockSpec(memory_space=pl.ANY)
    return pl.pallas_call(
        kernel,
        out_shape=out_shape,
        in_specs=[anywhere if k in hbm else vmem for k in range(len(arrays))],
        out_specs=jax.tree.map(lambda _: vmem, out_shape),
        scratch_shapes=scratch,
        compiler_params=pltpu.CompilerParams(vmem_limit_bytes=limit * 2**20),
    )(*arrays)


def struct(shape, dtype=bf16):
    return jax.ShapeDtypeStruct(shape, dtype)


def in_hbm(array):
    return pltpu.with_memory_space_constraint(array, pltpu.HBM)


def exchange(array, axes):
    return lax.all_to_all(array, axes, 0, 0, tiled=True)


def swap(array):
    return lax.ppermute(array, "core", [(0, 1), (1, 0)])


def body(
    queries,
    fresh_entries,
    page_cache,
    lengths,
    page_holder,
    page_slot,
    tokens,
    norm_gain,
    out_weight,
    expert_ids,
    gate_values,
    gate_weight,
    up_weight,
    down_weight,
):
    gain = norm_gain.reshape(1, D)
    holders = page_holder.T

    lines = DP * GROUPS * PMAX
    selected = call(
        select_kernel, struct((lines, HEAD)), (in_hbm(queries), in_hbm(holders))
    )
    asked = exchange(selected.reshape(DP, GROUPS * PMAX, HEAD), "dp").reshape(lines, HEAD)
    spread, live, gather, order, picks, scatter, weights, early = call(
        prepare_kernel,
        (
            struct((TOTAL, HEAD)),
            struct((TOTAL, HEAD), f32),
            struct((TOTAL, 2 * TOTAL)),
            struct((TOTAL, TOTAL)),
            struct((NX * ROWS, TOTAL)),
            struct((TOTAL, ROWS)),
            struct((ROWS, HEAD), f32),
            struct((EARLY * STEP, *page_cache.shape[2:])),
        ),
        (
            selected,
            in_hbm(holders),
            in_hbm(page_slot.T),
            in_hbm(lengths.reshape(1, TOTAL)),
            in_hbm(expert_ids.T),
            in_hbm(gate_values.T),
            in_hbm(page_cache),
        ),
        scratch=[pltpu.SemaphoreType.DMA(())],
        hbm=(0, 6),
    )
    parts = call(
        attend_kernel,
        struct((TOTAL, HEAD)),
        (asked, spread, live, gather, early, in_hbm(page_cache)),
        scratch=[
            pltpu.VMEM((2 * TOTAL, HEAD), f32),
            pltpu.VMEM(((STEPS - EARLY) * STEP, *page_cache.shape[2:]), bf16),
            pltpu.SemaphoreType.DMA((STEPS - EARLY,)),
        ],
        hbm=(5,),
    )
    parts = exchange(parts.reshape(HOLDERS, 8, HEAD), ("dp", "mp")).reshape(TOTAL, HEAD)

    half = struct((CHIPS // 2, SEQ, COLS))
    part_a, attended = call(
        project_kernel,
        (half, struct((SEQ, HEAD))),
        (parts, queries, fresh_entries, order, out_weight),
    )
    swapped_a = swap(part_a)
    part_b = call(project_late_kernel, half, (attended, out_weight))
    projected = call(
        core_sum_kernel,
        struct((CHIPS, SEQ, COLS)),
        (part_a, part_b, swapped_a, swap(part_b)),
    )
    projected = exchange(projected, ("x", "mp"))

    gained, plain = call(
        residual_kernel,
        (struct((DP, SEQ, COLS)), struct((NX, NC * MP, COLS), f32)),
        (projected, tokens, gain),
    )
    gained = exchange(gained, "dp").reshape(TOTAL, COLS)
    picked = call(pick_kernel, struct((CHIPS, ROWS, COLS)), (gained, picks))
    rows = exchange(picked, ("x", "mp"))
    other_out, own_hidden = call(
        hidden_kernel,
        (struct((CHIPS, ROWS, COLS)), struct((ROWS, FF))),
        (rows, gain, gate_weight, up_weight, scatter, weights, down_weight),
    )
    passed = swap(other_out)
    own_out = call(down_kernel, struct((CHIPS, ROWS, COLS)), (own_hidden, down_weight))

    summed = call(join_kernel, struct((CHIPS, ROWS, COLS)), (own_out, passed, plain))
    summed = exchange(summed, ("x", "mp"))
    lines = call(chip_sum_kernel, struct((DP, D // HEAD, HEAD)), (summed,))
    lines = exchange(lines, "dp")
    return call(final_kernel, struct((1, D)), (lines,))


def solution(mesh):
    fine = Mesh(mesh.devices.reshape(DP, NX, NC, MP), ("dp", "x", "core", "mp"))
    expert = ("x", "core")
    return jax.shard_map(
        body,
        mesh=fine,
        in_specs=(
            P("dp", expert),
            P(None, "dp", expert),
            P(expert, ("dp", "mp"), None, None, None),
            P(),
            P(),
            P(),
            P("dp", None),
            P(),
            P((*expert, "mp"), None),
            P(),
            P(),
            P(expert, None, ("dp", "mp")),
            P(expert, None, ("dp", "mp")),
            P(expert, ("dp", "mp"), None),
        ),
        out_specs=P(("dp", *expert, "mp"), None),
        check_vma=False,
    )
```
